32 devices in a mesh: seq: 2 (over x), tensor: 4 (over z), bucket: 4 (over y, core).
Axes of the slice: x: 2, y: 2, z: 4, core: 2. Of those that a mesh axis runs over, the one named last changes fastest.
Arguments:
- queries: bfloat16 [4, 1024, 3072], P('bucket', ('seq', 'tensor')), may hold values from -6 to 6
- keys: bfloat16 [4, 1024, 3072], P('bucket', ('seq', 'tensor')), may hold values from -6 to 6
- values: bfloat16 [4, 1024, 3072], P('bucket', ('seq', 'tensor')), may hold values from -6 to 6
- lengths: int32 [4], P('bucket'), may hold values from 256 to 1024, as said below
- out_weight: bfloat16 [3072, 3072], P(('seq', 'bucket'), 'tensor'), may hold values from -0.109375 to 0.109375
Outputs:
- projected: bfloat16 [4, 1024, 3072], P('bucket', ('seq', 'tensor'))
The draws below stay inside these ranges and needn't reach their ends.
Inputs may be any that keep to these rules, and one draw needn't show every extreme that they name: `lengths`: each bucket has 256 to 1024 live tokens, and at least one bucket has all 1024.
All inputs are finite; a program needn't handle non-finite values.
Results may differ from the reference program's by a relative error of at most 0.018.
Values may be sent and summed in bfloat16 or wider, within the bound.
A program may use at most 128 MiB of HBM per device.

```python
import jax
import jax.numpy as jnp
from jax import lax

D = 3072
HEADS = 24
HS = 128
LEN = 1024
BUCKETS = 4


def draw_queries(key, part):
    drawn = jax.random.normal(jax.random.fold_in(key, 1), (BUCKETS, LEN, D), jnp.float32)
    return jnp.clip(drawn, -6.0, 6.0).astype(jnp.bfloat16)


def draw_keys(key, part):
    drawn = jax.random.normal(jax.random.fold_in(key, 2), (BUCKETS, LEN, D), jnp.float32)
    return jnp.clip(drawn, -6.0, 6.0).astype(jnp.bfloat16)


def draw_lengths(key, part):
    drawn = jax.random.randint(jax.random.fold_in(key, 3), (BUCKETS,), LEN // 4, LEN + 1)
    fullest = jax.random.randint(jax.random.fold_in(key, 4), (), 0, BUCKETS)
    return jnp.where(jnp.arange(BUCKETS) == fullest, LEN, drawn).astype(jnp.int32)


def block_levels(rng, dims, pieces, low, top_value):
    level, own = 1.0, jax.random.fold_in(rng, 6)
    for position, parts in pieces:
        steps = jnp.exp(jax.random.uniform(jax.random.fold_in(own, position), (parts,), jnp.float32, low / len(pieces), top_value / len(pieces)))
        level = level * jnp.repeat(steps, dims[position] // parts).reshape([-1 if axis == position else 1 for axis in range(len(dims))])
    return level


def gaussian(rng, extent, width, limit, cuts=(), held_as=jnp.bfloat16):
    result = jax.random.normal(rng, extent, jnp.float32) * width
    if len(cuts) > 0:
        result = block_levels(rng, extent, cuts, -0.22, 0.18) * result
    return jnp.clip(result, min=-limit, max=limit).astype(held_as)


def setup_inputs(seed: int = 0) -> dict:
    key_list = jax.random.split(jax.random.key(seed), 6)
    queries = draw_queries(jax.random.fold_in(key_list[5], 71), 0)
    keys = draw_keys(jax.random.fold_in(key_list[5], 71), 0)
    values = gaussian(key_list[2], (BUCKETS, LEN, D), 1.0, 6.0, ((0, 4), (1, 8)))
    lengths = draw_lengths(jax.random.fold_in(key_list[5], 71), 0)
    out_weight = gaussian(key_list[4], (D, D), D ** -0.5, 0.109375, ((0, 8), (1, 4)))
    return {"queries": queries, "keys": keys, "values": values, "lengths": lengths, "out_weight": out_weight}


MASKED_SCORE = -1e30


def attend_head(query_head, key_head, value_head, usable):
    scores = jnp.dot(query_head, key_head.T, preferred_element_type=jnp.float32) * (HS ** -0.5)
    scores = jnp.where(usable[None, :], scores, MASKED_SCORE)
    row_peak = jnp.max(scores, axis=-1, keepdims=True)
    exponent = jnp.where(usable[None, :], jnp.exp(scores - row_peak), 0.0)
    numerator = jnp.dot(exponent.astype(jnp.bfloat16), value_head, preferred_element_type=jnp.float32)
    return numerator / jnp.sum(exponent, axis=-1, keepdims=True)


def reference(queries, keys, values, lengths, out_weight):
    def split_heads(array):
        return array.reshape(LEN, HEADS, HS).transpose(1, 0, 2)

    def one_bucket(inputs):
        bucket_q, bucket_k, bucket_v, live_len = inputs
        positions = jnp.arange(LEN, dtype=jnp.int32)
        usable = positions < live_len

        def one_head(trio):
            return attend_head(trio[0], trio[1], trio[2], usable)

        attended = lax.map(one_head, (split_heads(bucket_q), split_heads(bucket_k), split_heads(bucket_v)))
        mixed = attended.transpose(1, 0, 2).reshape(LEN, D)
        mixed = jnp.where(usable[:, None], mixed, 0.0).astype(jnp.bfloat16)
        return jnp.dot(mixed, out_weight, preferred_element_type=jnp.float32).astype(jnp.bfloat16)

    return lax.map(one_bucket, (queries, keys, values, lengths))
```

```python
import functools
import math

import jax
import jax.numpy as jnp
from jax import lax
from jax.experimental import pallas as pl
from jax.experimental.pallas import tpu as pltpu
from jax.sharding import PartitionSpec as P

HS = 128


MASKED_SCORE = -1e30


CHUNKS = 2


def shards(queries, keys, values, lengths, out_weight):
    tok_rows = queries.shape[1]
    n_tensor = lax.axis_size("tensor")
    tensor_index = lax.axis_index("tensor")
    live_len = lengths[0]
    local_q, local_k, local_v = (
        lax.all_to_all(queries[0], "seq", split_axis=1, concat_axis=0, tiled=True),
        lax.all_to_all(keys[0], "seq", split_axis=1, concat_axis=0, tiled=True),
        lax.all_to_all(values[0], "seq", split_axis=1, concat_axis=0, tiled=True),
    )
    row_count, col_count = local_q.shape
    head_count = col_count // HS
    query_heads = local_q.reshape(row_count, head_count, HS)

    def spots(first_row, total_rows):
        index_row = first_row + jnp.arange(total_rows, dtype=jnp.int32)
        owner = index_row // row_count
        within = index_row % row_count
        return (within // tok_rows * n_tensor + owner) * tok_rows + within % tok_rows

    query_usable = spots(tensor_index * row_count, row_count) < live_len
    initial = (
        jnp.full((row_count, head_count), MASKED_SCORE, jnp.float32),
        jnp.zeros((row_count, head_count), jnp.float32),
        jnp.zeros((row_count, head_count, HS), jnp.float32),
    )
    carried = initial
    first_row = jnp.int32(0)
    key_rows = lax.all_gather(local_k, "tensor", axis=0, tiled=True)
    value_rows = lax.all_gather(local_v, "tensor", axis=0, tiled=True)
    for offset in range(key_rows.shape[0] // row_count):
        row_peak, row_sum, accumulated = carried
        key_tile = key_rows[offset * row_count : (offset + 1) * row_count].reshape(
            row_count, head_count, HS
        )
        value_tile = value_rows[offset * row_count : (offset + 1) * row_count].reshape(
            row_count, head_count, HS
        )
        key_usable = spots(first_row + offset * row_count, row_count) < live_len
        scores = jnp.einsum(
            "qhd,khd->qhk", query_heads, key_tile, preferred_element_type=jnp.float32
        ) * HS ** (-0.5)
        scores = jnp.where(key_usable[None, None, :], scores, MASKED_SCORE)
        peak_new = jnp.maximum(row_peak, jnp.max(scores, axis=-1))
        exponent = jnp.where(key_usable[None, None, :], jnp.exp(scores - peak_new[..., None]), 0.0)
        rescale = jnp.exp(row_peak - peak_new)
        accumulated = accumulated * rescale[..., None] + jnp.einsum(
            "qhk,khd->qhd",
            exponent.astype(jnp.bfloat16),
            value_tile,
            preferred_element_type=jnp.float32,
        )
        carried = (peak_new, row_sum * rescale + jnp.sum(exponent, axis=-1), accumulated)
    row_peak, row_sum, accumulated = carried
    attended = accumulated / row_sum[..., None]
    mixed = jnp.where(query_usable[:, None], attended.reshape(row_count, col_count), 0.0).astype(
        jnp.bfloat16
    )
    restored = lax.all_to_all(mixed, "seq", split_axis=0, concat_axis=1, tiled=True)
    wide_weight = lax.all_gather(out_weight, "tensor", axis=1, tiled=True)
    summed = jnp.dot(
        restored,
        lax.all_gather(wide_weight, ("seq", "bucket"), axis=0, tiled=True),
        preferred_element_type=jnp.float32,
    )
    return summed.astype(jnp.bfloat16)[None]


def whole_kernel(
    axes, sizes, len_ref, q_ref, k_ref, v_ref, w_ref, out_ref,
    held, got, done, mixed, weight, part_out, part_in, own_part, load_sem, own_sem,
    qkv_send, qkv_recv, att_send, att_recv, up_send, down_send, line_recv,
    far_send, far_recv, near_send, near_recv, part_send, part_recv, out_sem,
):
    n_seq, n_tensor, n_bucket = sizes
    s, t, b = lax.axis_index("seq"), lax.axis_index("tensor"), lax.axis_index("bucket")
    group = n_seq * n_tensor
    rows = q_ref.shape[1]
    width = q_ref.shape[2]
    heads = width // HS // group
    w_rows, w_cols = w_ref.shape
    live = len_ref[0]

    def device(ds, dt, db):
        place = {"seq": ds, "tensor": dt, "bucket": db}
        return tuple(place[name] for name in axes)

    def remote(src, dst, send, recv, where):
        return pltpu.make_async_remote_copy(
            src_ref=src, dst_ref=dst, send_sem=send, recv_sem=recv,
            device_id=where, device_id_type=pl.DeviceIdType.MESH,
        )

    me = s * n_tensor + t
    streams = (q_ref, k_ref, v_ref)
    barrier = pltpu.get_barrier_semaphore()

    def spot(place):
        return pl.ds(pl.multiple_of(place * rows, rows), rows)

    def peer_of(e):
        return (s + e // n_tensor) % 2, (t + e % n_tensor) % n_tensor

    def source_of(e):
        return (s + e // n_tensor) % 2, (t + n_tensor - e % n_tensor) % n_tensor

    def qkv_copy(h, j, e, to, source):
        cols = pl.ds(pl.multiple_of(((to[0] * n_tensor + to[1]) * heads + h) * HS, HS), HS)
        return remote(
            held.at[j, :, cols],
            got.at[h, j, spot(source[0] * n_tensor + source[1]), :],
            qkv_send.at[h, j, e],
            qkv_recv.at[h, j, e],
            device(to[0], to[1], b),
        )

    def start_stream(h, js, first, last):
        def body(e, carry):
            for j in js:
                qkv_copy(h, j, e, peer_of(e), (s, t)).start()
            return carry

        lax.fori_loop(first, last, body, 0)

    def arrive(h, js, first, last):
        def body(e, carry):
            for j in js:
                qkv_copy(h, j, e, (s, t), source_of(e)).wait_recv()
            return carry

        lax.fori_loop(first, last, body, 0)

    def own_arrive(h):
        for j in range(3):
            own_copy(h, j).wait()

    def start_across(h):
        start_stream(h, (1, 2, 0), n_tensor, n_tensor + 1)

    def start_kv_far(h, first=1, last=4):
        start_stream(h, (1, 2), first, last)
        start_stream(h, (1, 2, 0), n_tensor + first, n_tensor + last)


    def start_own(h):
        start_stream(h, (0,), 1, n_tensor)

    chunk = w_rows // CHUNKS

    def piece(row_block, col_block, c):
        return weight.at[
            pl.ds(pl.multiple_of(row_block * w_rows + c * chunk, chunk), chunk),
            pl.ds(pl.multiple_of(col_block * w_cols, w_cols), w_cols),
        ]

    far, near = (b + 2) % 4, b + 1 - 2 * (b % 2)

    def up_copy(p, c):
        return remote(
            piece(b, p, c), piece(b, p, c), up_send.at[p, c], line_recv.at[p, c], device(s, t + 1, b)
        )

    def down_copy(p, c):
        return remote(
            piece(b, p, c), piece(b, p, c), down_send.at[p, c], line_recv.at[p, c], device(s, t - 1, b)
        )

    def far_copy(p, c, row_block):
        return remote(
            piece(row_block, p, c), piece(row_block, p, c), far_send.at[p, c], far_recv.at[p, c], device(s, t, far)
        )

    def near_copy(k, p, c, row_block):
        return remote(
            piece(row_block, p, c), piece(row_block, p, c),
            near_send.at[k, p, c], near_recv.at[k, p, c], device(s, t, near),
        )

    def spread(p, c):
        far_copy(p, c, b).start()
        near_copy(0, p, c, b).start()

    def relay_chunk(k, c):
        @pl.when(t >= k)
        def _():
            up_copy(t - k, c).wait_recv()

            @pl.when(t < n_tensor - 1)
            def _():
                up_copy(t - k, c).start()

            spread(t - k, c)

        @pl.when(t + k < n_tensor)
        def _():
            down_copy(t + k, c).wait_recv()

            @pl.when(t > 0)
            def _():
                down_copy(t + k, c).start()

            spread(t + k, c)

    def relay(k):
        for c in range(CHUNKS):
            relay_chunk(k, c)

    own_piece = weight.at[
        pl.ds(pl.multiple_of(b * w_rows, w_rows), w_rows),
        pl.ds(pl.multiple_of(t * w_cols, w_cols), w_cols),
    ]
    weight_load = pltpu.make_async_copy(w_ref, own_piece, load_sem.at[3])
    weight_load.start()

    def load(j):
        return pltpu.make_async_copy(streams[j].at[0], held.at[j], load_sem.at[j])

    def own_copy(h, j):
        cols = pl.ds(pl.multiple_of((me * heads + h) * HS, HS), HS)
        return pltpu.make_async_copy(streams[j].at[0, :, cols], got.at[h, j, spot(me), :], own_sem.at[h, j])

    def greet(where):
        pl.semaphore_signal(barrier, inc=1, device_id=where, device_id_type=pl.DeviceIdType.MESH)

    for e in range(1, group):
        to = peer_of(e)
        greet(device(to[0], to[1], b))
    greet(device(s, t, far))
    greet(device(s, t, near))
    for j in (1, 2, 0):
        load(j).start()
    for h in range(heads):
        for j in range(3):
            own_copy(h, j).start()
    pl.semaphore_wait(barrier, group + 1)
    weight_load.wait()

    for c in range(CHUNKS):
        @pl.when(t < n_tensor - 1)
        def _():
            up_copy(t, c).start()

        @pl.when(t > 0)
        def _():
            down_copy(t, c).start()

        spread(t, c)
    for j in (1, 2, 0):
        load(j).wait()

    upper = t // 2
    order = (t, 1 - t + 4 * upper, 2 - upper, 3 - 3 * upper)

    def forward(p):
        for c in range(CHUNKS):
            far_copy(p, c, far).wait_recv()
            near_copy(1, p, c, far).start()

    total = group * rows
    usable = lax.broadcasted_iota(jnp.int32, (1, total), 1) < live
    factor = HS ** (-0.5) * math.log2(math.e)

    def att_copy(h, f, d, target, source):
        cols = pl.ds(pl.multiple_of((source * heads + h) * HS, HS), HS)
        return remote(
            done.at[h, spot((s + f) % 2 * n_tensor + target), :], mixed.at[f, :, cols],
            att_send.at[h, f, d], att_recv.at[h, f, d], device(s, target, b),
        )

    def attend_rows(h, query, own_token):
        scores = lax.dot_general(
            query, got[h, 1], (((1,), (1,)), ((), ())), preferred_element_type=jnp.float32
        )
        scores = jnp.where(usable, scores, MASKED_SCORE)
        peak = jnp.max(scores, axis=-1, keepdims=True)
        expo = jnp.exp2((scores - peak) * factor)
        denominator = jnp.sum(expo, axis=-1, keepdims=True)
        result = jnp.dot(expo.astype(jnp.bfloat16), got[h, 2], preferred_element_type=jnp.float32) / denominator
        return jnp.where(own_token < live, result, 0.0).astype(jnp.bfloat16)

    def attend(h, f):
        side = (s + f) % 2 * n_tensor
        row = lax.broadcasted_iota(jnp.int32, (rows, 1), 0)
        for step in range(0, n_tensor, 2):
            targets = [(t + step + i) % n_tensor for i in (1, 2)]
            spans = [spot(side + target) for target in targets]
            result = attend_rows(
                h,
                jnp.concatenate([got[h, 0, span, :] for span in spans], axis=0),
                jnp.concatenate([(side + target) * rows + row for target in targets], axis=0),
            )
            for i in range(2):
                d = step + i + 1
                if d < n_tensor:
                    done[h, spans[i], :] = result[i * rows : (i + 1) * rows]
                    att_copy(h, f, d, targets[i], t).start()
                else:
                    mixed[f, :, pl.ds(pl.multiple_of((t * heads + h) * HS, HS), HS)] = result[
                        i * rows : (i + 1) * rows
                    ]

    def back(h, f):
        def body(d, carry):
            att_copy(h, f, d, t, (t + n_tensor - d) % n_tensor).wait_recv()
            return carry

        lax.fori_loop(1, n_tensor, body, 0)

    def cut_of(p):
        return pl.ds(pl.multiple_of(p * w_cols, w_cols), w_cols)

    def part_copy(p):
        cut = cut_of(p)
        return remote(
            part_out.at[:, cut], part_in.at[:, cut], part_send.at[p], part_recv.at[p], device(1 - s, t, b)
        )

    def leave(p):
        cut = cut_of(p)
        return pltpu.make_async_copy(part_in.at[:, cut], out_ref.at[0, :, cut], out_sem.at[p])

    def project_far(k):
        p = order[k]
        for c in range(CHUNKS):
            near_copy(0, p, c, near).wait_recv()
            near_copy(1, p, c, (near + 2) % 4).wait_recv()
        cut = cut_of(p)
        part_out[:, cut] = jnp.dot(
            mixed[1], weight[:, cut], preferred_element_type=jnp.float32
        ).astype(jnp.bfloat16)
        part_copy(p).start()

    for h in range(heads):
        start_across(h)

    relay(1)
    middle = ((t == 1) | (t == 2)).astype(jnp.int32)
    inner_first = jnp.where(t == 2, 2, 1)
    inner_last = inner_first + 2 * middle
    outer_first = jnp.where(t == 1, 3, 1)
    outer_last = jnp.where(t == 2, 2, 4)
    for h in range(heads):
        start_kv_far(h, inner_first, inner_last)
    forward(order[0])
    relay(2)
    for h in range(heads):
        start_kv_far(h, outer_first, outer_last)
    forward(order[1])
    relay(3)

    for h in range(heads):
        own_arrive(h)
        arrive(h, (1, 2), 1, group)
        arrive(h, (0,), n_tensor, group)
        attend(h, 1)
        if h == 0:
            forward(order[2])
            start_own(0)
        if h == 1:
            forward(order[3])
        if h == 2:
            start_own(1)
            start_own(2)
    arrive(0, (0,), 1, n_tensor)
    attend(0, 0)
    for h in range(heads):
        back(h, 1)
    project_far(0)
    project_far(1)
    arrive(1, (0,), 1, n_tensor)
    attend(1, 0)
    project_far(2)
    project_far(3)
    arrive(2, (0,), 1, n_tensor)
    attend(2, 0)
    for h in range(heads):
        back(h, 0)
    for p in order:
        cut = cut_of(p)
        own_part[:, cut] = jnp.dot(mixed[0], weight[:, cut], preferred_element_type=jnp.float32)
    for p in order:
        cut = cut_of(p)
        part_copy(p).wait_recv()
        part_in[:, cut] = (own_part[:, cut] + part_in[:, cut].astype(jnp.float32)).astype(jnp.bfloat16)
        leave(p).start()

    for h in range(heads):
        def sent(e, carry):
            for j in range(3):
                qkv_copy(h, j, e, peer_of(e), (s, t)).wait_send()
            return carry

        lax.fori_loop(1, group, sent, 0)

        def att_sent(d, carry):
            for f in range(2):
                att_copy(h, f, d, (t + d) % n_tensor, t).wait_send()
            return carry

        lax.fori_loop(1, n_tensor, att_sent, 0)
    for c in range(CHUNKS):
        for k in range(n_tensor):
            @pl.when((t >= k) & (t < n_tensor - 1))
            def _():
                up_copy(t - k, c).wait_send()

            @pl.when((t + k < n_tensor) & (t > 0))
            def _():
                down_copy(t + k, c).wait_send()

        for p in range(n_tensor):
            far_copy(p, c, b).wait_send()
            near_copy(0, p, c, b).wait_send()
            near_copy(1, p, c, far).wait_send()

    for p in range(n_tensor):
        part_copy(p).wait_send()
        leave(p).wait()


def fused(axes, sizes, queries, keys, values, lengths, out_weight):
    n_seq, n_tensor, n_bucket = sizes
    rows, width = queries.shape[1:]
    group = n_seq * n_tensor
    heads = width // HS // group
    total = group * rows
    half = width // n_seq
    anywhere = pl.BlockSpec(memory_space=pl.ANY)
    dma = pltpu.SemaphoreType.DMA
    return pl.pallas_call(
        functools.partial(whole_kernel, axes, sizes),
        out_shape=jax.ShapeDtypeStruct(queries.shape, queries.dtype),
        in_specs=[pl.BlockSpec(memory_space=pltpu.SMEM), anywhere, anywhere, anywhere, anywhere],
        out_specs=anywhere,
        scratch_shapes=[
            pltpu.VMEM((3, rows, width), jnp.bfloat16),
            pltpu.VMEM((heads, 3, total, HS), jnp.bfloat16),
            pltpu.VMEM((heads, total, HS), jnp.bfloat16),
            pltpu.VMEM((n_seq, rows, half), jnp.bfloat16),
            pltpu.VMEM((half, width), jnp.bfloat16),
            pltpu.VMEM((rows, width), jnp.bfloat16),
            pltpu.VMEM((rows, width), jnp.bfloat16),
            pltpu.VMEM((rows, width), jnp.float32),
            dma((4,)),
            dma((heads, 3)),
            dma((heads, 3, group)),
            dma((heads, 3, group)),
            dma((heads, 2, n_tensor)),
            dma((heads, 2, n_tensor)),
            dma((n_tensor, CHUNKS)),
            dma((n_tensor, CHUNKS)),
            dma((n_tensor, CHUNKS)),
            dma((n_tensor, CHUNKS)),
            dma((n_tensor, CHUNKS)),
            dma((2, n_tensor, CHUNKS)),
            dma((2, n_tensor, CHUNKS)),
            dma((n_tensor,)),
            dma((n_tensor,)),
            dma((n_tensor,)),
        ],
        compiler_params=pltpu.CompilerParams(
            collective_id=0, has_side_effects=True, vmem_limit_bytes=56 * 1024 * 1024,
        ),
    )(lengths, queries, keys, values, out_weight)


def solution(mesh):
    in_specs = (
        P("bucket", ("seq", "tensor"), None),
        P("bucket", ("seq", "tensor"), None),
        P("bucket", ("seq", "tensor"), None),
        P("bucket"),
        P(("seq", "bucket"), "tensor"),
    )
    out_specs = P("bucket", ("seq", "tensor"), None)
    sizes = tuple(mesh.shape[name] for name in ("seq", "tensor", "bucket"))

    def step(queries, keys, values, lengths, out_weight):
        head_count = queries.shape[2] // HS
        fits = sizes[0] == 2 and sizes[1] == sizes[2] == 4 and head_count % (sizes[0] * sizes[1]) == 0
        if fits:
            return fused(mesh.axis_names, sizes, queries, keys, values, lengths, out_weight)
        return shards(queries, keys, values, lengths, out_weight)

    return jax.shard_map(step, mesh=mesh, in_specs=in_specs, out_specs=out_specs, check_vma=False)
```

```python
import functools
import math

import jax
import jax.numpy as jnp
from jax import lax
from jax.experimental import pallas as pl
from jax.experimental.pallas import tpu as pltpu
from jax.sharding import PartitionSpec as P

HS = 128


MASKED_SCORE = -1e30


def shards(queries, keys, values, lengths, out_weight):
    tok_rows = queries.shape[1]
    n_tensor = lax.axis_size("tensor")
    tensor_index = lax.axis_index("tensor")
    live_len = lengths[0]
    local_q, local_k, local_v = (
        lax.all_to_all(queries[0], "seq", split_axis=1, concat_axis=0, tiled=True),
        lax.all_to_all(keys[0], "seq", split_axis=1, concat_axis=0, tiled=True),
        lax.all_to_all(values[0], "seq", split_axis=1, concat_axis=0, tiled=True),
    )
    row_count, col_count = local_q.shape
    head_count = col_count // HS
    query_heads = local_q.reshape(row_count, head_count, HS)

    def spots(first_row, total_rows):
        index_row = first_row + jnp.arange(total_rows, dtype=jnp.int32)
        owner = index_row // row_count
        within = index_row % row_count
        return (within // tok_rows * n_tensor + owner) * tok_rows + within % tok_rows

    query_usable = spots(tensor_index * row_count, row_count) < live_len
    initial = (
        jnp.full((row_count, head_count), MASKED_SCORE, jnp.float32),
        jnp.zeros((row_count, head_count), jnp.float32),
        jnp.zeros((row_count, head_count, HS), jnp.float32),
    )
    carried = initial
    first_row = jnp.int32(0)
    key_rows = lax.all_gather(local_k, "tensor", axis=0, tiled=True)
    value_rows = lax.all_gather(local_v, "tensor", axis=0, tiled=True)
    for offset in range(key_rows.shape[0] // row_count):
        row_peak, row_sum, accumulated = carried
        key_tile = key_rows[offset * row_count : (offset + 1) * row_count].reshape(
            row_count, head_count, HS
        )
        value_tile = value_rows[offset * row_count : (offset + 1) * row_count].reshape(
            row_count, head_count, HS
        )
        key_usable = spots(first_row + offset * row_count, row_count) < live_len
        scores = jnp.einsum(
            "qhd,khd->qhk", query_heads, key_tile, preferred_element_type=jnp.float32
        ) * HS ** (-0.5)
        scores = jnp.where(key_usable[None, None, :], scores, MASKED_SCORE)
        peak_new = jnp.maximum(row_peak, jnp.max(scores, axis=-1))
        exponent = jnp.where(key_usable[None, None, :], jnp.exp(scores - peak_new[..., None]), 0.0)
        rescale = jnp.exp(row_peak - peak_new)
        accumulated = accumulated * rescale[..., None] + jnp.einsum(
            "qhk,khd->qhd",
            exponent.astype(jnp.bfloat16),
            value_tile,
            preferred_element_type=jnp.float32,
        )
        carried = (peak_new, row_sum * rescale + jnp.sum(exponent, axis=-1), accumulated)
    row_peak, row_sum, accumulated = carried
    attended = accumulated / row_sum[..., None]
    mixed = jnp.where(query_usable[:, None], attended.reshape(row_count, col_count), 0.0).astype(
        jnp.bfloat16
    )
    restored = lax.all_to_all(mixed, "seq", split_axis=0, concat_axis=1, tiled=True)
    wide_weight = lax.all_gather(out_weight, "tensor", axis=1, tiled=True)
    summed = jnp.dot(
        restored,
        lax.all_gather(wide_weight, ("seq", "bucket"), axis=0, tiled=True),
        preferred_element_type=jnp.float32,
    )
    return summed.astype(jnp.bfloat16)[None]


def whole_kernel(
    axes, sizes, len_ref, q_ref, k_ref, v_ref, w_ref, out_ref,
    held, got, done, mixed, weight, part_out, part_in, own_part, load_sem, own_sem,
    qkv_send, qkv_recv, att_send, att_recv, up_send, down_send, line_recv,
    far_send, far_recv, near_send, near_recv, part_send, part_recv,
):
    n_seq, n_tensor, n_bucket = sizes
    s, t, b = lax.axis_index("seq"), lax.axis_index("tensor"), lax.axis_index("bucket")
    group = n_seq * n_tensor
    rows = q_ref.shape[1]
    width = q_ref.shape[2]
    heads = width // HS // group
    w_rows, w_cols = w_ref.shape
    live = len_ref[0]

    def device(ds, dt, db):
        place = {"seq": ds, "tensor": dt, "bucket": db}
        return tuple(place[name] for name in axes)

    def remote(src, dst, send, recv, where):
        return pltpu.make_async_remote_copy(
            src_ref=src, dst_ref=dst, send_sem=send, recv_sem=recv,
            device_id=where, device_id_type=pl.DeviceIdType.MESH,
        )

    me = s * n_tensor + t
    streams = (q_ref, k_ref, v_ref)
    barrier = pltpu.get_barrier_semaphore()

    def spot(place):
        return pl.ds(pl.multiple_of(place * rows, rows), rows)

    def peer_of(e):
        return (s + e // n_tensor) % 2, (t + e % n_tensor) % n_tensor

    def source_of(e):
        return (s + e // n_tensor) % 2, (t + n_tensor - e % n_tensor) % n_tensor

    def qkv_copy(h, j, e, to, source):
        cols = pl.ds(pl.multiple_of(((to[0] * n_tensor + to[1]) * heads + h) * HS, HS), HS)
        return remote(
            held.at[j, :, cols],
            got.at[h, j, spot(source[0] * n_tensor + source[1]), :],
            qkv_send.at[h, j, e],
            qkv_recv.at[h, j, e],
            device(to[0], to[1], b),
        )

    def start_stream(h, js, first, last):
        def body(e, carry):
            for j in js:
                qkv_copy(h, j, e, peer_of(e), (s, t)).start()
            return carry

        lax.fori_loop(first, last, body, 0)

    def arrive(h, js, first, last):
        def body(e, carry):
            for j in js:
                qkv_copy(h, j, e, (s, t), source_of(e)).wait_recv()
            return carry

        lax.fori_loop(first, last, body, 0)

    def own_arrive(h):
        for j in range(3):
            own_copy(h, j).wait()

    def start_across(h):
        start_stream(h, (1, 2, 0), n_tensor, n_tensor + 1)

    def start_kv_far(h, first=1, last=4):
        start_stream(h, (1, 2), first, last)
        start_stream(h, (1, 2, 0), n_tensor + first, n_tensor + last)


    def start_own(h):
        start_stream(h, (0,), 1, n_tensor)

    def piece(row_block, col_block, c):
        return weight.at[
            c,
            pl.ds(pl.multiple_of(row_block * HS, HS), HS),
            pl.ds(pl.multiple_of(col_block * w_cols, w_cols), w_cols),
        ]

    far, near = (b + 2) % 4, b + 1 - 2 * (b % 2)

    def up_copy(p, c):
        return remote(
            piece(b, p, c), piece(b, p, c), up_send.at[p, c], line_recv.at[p, c], device(s, t + 1, b)
        )

    def down_copy(p, c):
        return remote(
            piece(b, p, c), piece(b, p, c), down_send.at[p, c], line_recv.at[p, c], device(s, t - 1, b)
        )

    def far_copy(p, c, row_block):
        return remote(
            piece(row_block, p, c), piece(row_block, p, c), far_send.at[p, c], far_recv.at[p, c], device(s, t, far)
        )

    def near_copy(k, p, c, row_block):
        return remote(
            piece(row_block, p, c), piece(row_block, p, c),
            near_send.at[k, p, c], near_recv.at[k, p, c], device(s, t, near),
        )

    def spread(p, c):
        far_copy(p, c, b).start()
        near_copy(0, p, c, b).start()

    def relay_chunk(k, c):
        @pl.when(t >= k)
        def _():
            up_copy(t - k, c).wait_recv()

            @pl.when(t < n_tensor - 1)
            def _():
                up_copy(t - k, c).start()

            spread(t - k, c)

        @pl.when(t + k < n_tensor)
        def _():
            down_copy(t + k, c).wait_recv()

            @pl.when(t > 0)
            def _():
                down_copy(t + k, c).start()

            spread(t + k, c)

    def relay(k):
        for c in range(heads):
            relay_chunk(k, c)

    def weight_load(c):
        return pltpu.make_async_copy(w_ref.at[pl.ds(c * HS, HS), :], piece(b, t, c), load_sem.at[3 + c])

    for c in range(heads):
        weight_load(c).start()

    def load(j):
        return pltpu.make_async_copy(streams[j].at[0], held.at[j], load_sem.at[j])

    def own_copy(h, j):
        cols = pl.ds(pl.multiple_of((me * heads + h) * HS, HS), HS)
        return pltpu.make_async_copy(streams[j].at[0, :, cols], got.at[h, j, spot(me), :], own_sem.at[h, j])

    def greet(where):
        pl.semaphore_signal(barrier, inc=1, device_id=where, device_id_type=pl.DeviceIdType.MESH)

    for e in range(1, group):
        to = peer_of(e)
        greet(device(to[0], to[1], b))
    greet(device(s, t, far))
    greet(device(s, t, near))
    for j in (1, 2, 0):
        load(j).start()
    for h in range(heads):
        for j in range(3):
            own_copy(h, j).start()
    pl.semaphore_wait(barrier, group + 1)
    for c in range(heads):
        weight_load(c).wait()

        @pl.when(t < n_tensor - 1)
        def _():
            up_copy(t, c).start()

        @pl.when(t > 0)
        def _():
            down_copy(t, c).start()

        spread(t, c)
    for j in (1, 2, 0):
        load(j).wait()

    upper = t // 2
    order = (t, 1 - t + 4 * upper, 2 - upper, 3 - 3 * upper)

    def forward(p):
        for c in range(heads):
            far_copy(p, c, far).wait_recv()
            near_copy(1, p, c, far).start()

    total = group * rows
    usable = lax.broadcasted_iota(jnp.int32, (1, total), 1) < live
    factor = HS ** (-0.5) * math.log2(math.e)

    def att_copy(h, f, d, target, source):
        cols = pl.ds(pl.multiple_of(source * HS, HS), HS)
        return remote(
            done.at[h, spot((s + f) % 2 * n_tensor + target), :], mixed.at[f, h, :, cols],
            att_send.at[h, f, d], att_recv.at[h, f, d], device(s, target, b),
        )

    def attend_rows(h, query, own_token):
        scores = lax.dot_general(
            query, got[h, 1], (((1,), (1,)), ((), ())), preferred_element_type=jnp.float32
        )
        scores = jnp.where(usable, scores, MASKED_SCORE)
        peak = jnp.max(scores, axis=-1, keepdims=True)
        expo = jnp.exp2((scores - peak) * factor)
        denominator = jnp.sum(expo, axis=-1, keepdims=True)
        result = jnp.dot(expo.astype(jnp.bfloat16), got[h, 2], preferred_element_type=jnp.float32) / denominator
        return jnp.where(own_token < live, result, 0.0).astype(jnp.bfloat16)

    def attend(h, f):
        side = (s + f) % 2 * n_tensor
        row = lax.broadcasted_iota(jnp.int32, (rows, 1), 0)
        for step in range(0, n_tensor, 2):
            targets = [(t + step + i) % n_tensor for i in (1, 2)]
            spans = [spot(side + target) for target in targets]
            result = attend_rows(
                h,
                jnp.concatenate([got[h, 0, span, :] for span in spans], axis=0),
                jnp.concatenate([(side + target) * rows + row for target in targets], axis=0),
            )
            for i in range(2):
                d = step + i + 1
                if d < n_tensor:
                    done[h, spans[i], :] = result[i * rows : (i + 1) * rows]
                    att_copy(h, f, d, targets[i], t).start()
                else:
                    mixed[f, h, :, pl.ds(pl.multiple_of(t * HS, HS), HS)] = result[
                        i * rows : (i + 1) * rows
                    ]

    def back(h, f):
        def body(d, carry):
            att_copy(h, f, d, t, (t + n_tensor - d) % n_tensor).wait_recv()
            return carry

        lax.fori_loop(1, n_tensor, body, 0)

    def cut_of(p):
        return pl.ds(pl.multiple_of(p * w_cols, w_cols), w_cols)

    def part_copy(p):
        cut = cut_of(p)
        return remote(
            part_out.at[:, cut], part_in.at[:, cut], part_send.at[p], part_recv.at[p], device(1 - s, t, b)
        )

    def product(f, h, cut):
        return jnp.dot(mixed[f, h], weight[h, :, cut], preferred_element_type=jnp.float32)

    def own_product(h):
        for p in order:
            cut = cut_of(p)
            own_part[:, cut] = product(0, h, cut) if h == 0 else own_part[:, cut] + product(0, h, cut)

    def finish(p):
        cut = cut_of(p)
        part_copy(p).wait_recv()
        out_ref[0, :, cut] = (own_part[:, cut] + part_in[:, cut].astype(jnp.float32)).astype(jnp.bfloat16)

    def project_far(k):
        p = order[k]
        for c in range(heads):
            near_copy(0, p, c, near).wait_recv()
            near_copy(1, p, c, (near + 2) % 4).wait_recv()
        cut = cut_of(p)
        part_out[:, cut] = sum(product(1, h, cut) for h in range(heads)).astype(jnp.bfloat16)
        part_copy(p).start()

    for h in range(heads):
        start_across(h)

    relay(1)
    middle = ((t == 1) | (t == 2)).astype(jnp.int32)
    inner_first = jnp.where(t == 2, 2, 1)
    inner_last = inner_first + 2 * middle
    outer_first = jnp.where(t == 1, 3, 1)
    outer_last = jnp.where(t == 2, 2, 4)
    for h in range(heads):
        start_kv_far(h, inner_first, inner_last)
    forward(order[0])
    relay(2)
    for h in range(heads):
        start_kv_far(h, outer_first, outer_last)
    forward(order[1])
    relay(3)

    for h in range(heads):
        own_arrive(h)
        arrive(h, (1, 2), 1, group)
        arrive(h, (0,), n_tensor, group)
        attend(h, 1)
        if h == 0:
            forward(order[2])
        if h == 1:
            forward(order[3])
            start_own(0)
    for h in range(heads):
        back(h, 1)
    start_own(1)
    start_own(2)
    project_far(0)
    arrive(0, (0,), 1, n_tensor)
    attend(0, 0)
    project_far(1)
    arrive(1, (0,), 1, n_tensor)
    attend(1, 0)
    project_far(2)
    arrive(2, (0,), 1, n_tensor)
    attend(2, 0)
    project_far(3)
    for h in range(heads):
        back(h, 0)
        own_product(h)
    for p in order:
        finish(p)

    for h in range(heads):
        def sent(e, carry):
            for j in range(3):
                qkv_copy(h, j, e, peer_of(e), (s, t)).wait_send()
            return carry

        lax.fori_loop(1, group, sent, 0)

        def att_sent(d, carry):
            for f in range(2):
                att_copy(h, f, d, (t + d) % n_tensor, t).wait_send()
            return carry

        lax.fori_loop(1, n_tensor, att_sent, 0)
    for c in range(heads):
        for k in range(n_tensor):
            @pl.when((t >= k) & (t < n_tensor - 1))
            def _():
                up_copy(t - k, c).wait_send()

            @pl.when((t + k < n_tensor) & (t > 0))
            def _():
                down_copy(t + k, c).wait_send()

        for p in range(n_tensor):
            far_copy(p, c, b).wait_send()
            near_copy(0, p, c, b).wait_send()
            near_copy(1, p, c, far).wait_send()

    for p in range(n_tensor):
        part_copy(p).wait_send()


def fused(axes, sizes, queries, keys, values, lengths, out_weight):
    n_seq, n_tensor, n_bucket = sizes
    rows, width = queries.shape[1:]
    group = n_seq * n_tensor
    heads = width // HS // group
    total = group * rows
    anywhere = pl.BlockSpec(memory_space=pl.ANY)
    dma = pltpu.SemaphoreType.DMA
    return pl.pallas_call(
        functools.partial(whole_kernel, axes, sizes),
        out_shape=jax.ShapeDtypeStruct(queries.shape, queries.dtype),
        in_specs=[pl.BlockSpec(memory_space=pltpu.SMEM), anywhere, anywhere, anywhere, anywhere],
        out_specs=pl.BlockSpec(memory_space=pltpu.VMEM),
        scratch_shapes=[
            pltpu.VMEM((3, rows, width), jnp.bfloat16),
            pltpu.VMEM((heads, 3, total, HS), jnp.bfloat16),
            pltpu.VMEM((heads, total, HS), jnp.bfloat16),
            pltpu.VMEM((n_seq, heads, rows, n_tensor * HS), jnp.bfloat16),
            pltpu.VMEM((heads, n_bucket * HS, width), jnp.bfloat16),
            pltpu.VMEM((rows, width), jnp.bfloat16),
            pltpu.VMEM((rows, width), jnp.bfloat16),
            pltpu.VMEM((rows, width), jnp.float32),
            dma((3 + heads,)),
            dma((heads, 3)),
            dma((heads, 3, group)),
            dma((heads, 3, group)),
            dma((heads, 2, n_tensor)),
            dma((heads, 2, n_tensor)),
            dma((n_tensor, heads)),
            dma((n_tensor, heads)),
            dma((n_tensor, heads)),
            dma((n_tensor, heads)),
            dma((n_tensor, heads)),
            dma((2, n_tensor, heads)),
            dma((2, n_tensor, heads)),
            dma((n_tensor,)),
            dma((n_tensor,)),
        ],
        compiler_params=pltpu.CompilerParams(
            collective_id=0, has_side_effects=True, vmem_limit_bytes=32 * 1024 * 1024,
        ),
    )(lengths, *(pltpu.with_memory_space_constraint(x, pltpu.HBM) for x in (queries, keys, values, out_weight)))


def solution(mesh):
    in_specs = (
        P("bucket", ("seq", "tensor"), None),
        P("bucket", ("seq", "tensor"), None),
        P("bucket", ("seq", "tensor"), None),
        P("bucket"),
        P(("seq", "bucket"), "tensor"),
    )
    out_specs = P("bucket", ("seq", "tensor"), None)
    sizes = tuple(mesh.shape[name] for name in ("seq", "tensor", "bucket"))

    def step(queries, keys, values, lengths, out_weight):
        head_count = queries.shape[2] // HS
        fits = sizes[0] == 2 and sizes[1] == sizes[2] == 4 and head_count % (sizes[0] * sizes[1]) == 0
        if fits:
            return fused(mesh.axis_names, sizes, queries, keys, values, lengths, out_weight)
        return shards(queries, keys, values, lengths, out_weight)

    return jax.shard_map(step, mesh=mesh, in_specs=in_specs, out_specs=out_specs, check_vma=False)
```

```python
import functools
import math

import jax
import jax.numpy as jnp
from jax import lax
from jax.experimental import pallas as pl
from jax.experimental.pallas import tpu as pltpu
from jax.sharding import PartitionSpec as P

HS = 128


MASKED_SCORE = -1e30


def shards(queries, keys, values, lengths, out_weight):
    tok_rows = queries.shape[1]
    n_tensor = lax.axis_size("tensor")
    tensor_index = lax.axis_index("tensor")
    live_len = lengths[0]
    local_q, local_k, local_v = (
        lax.all_to_all(queries[0], "seq", split_axis=1, concat_axis=0, tiled=True),
        lax.all_to_all(keys[0], "seq", split_axis=1, concat_axis=0, tiled=True),
        lax.all_to_all(values[0], "seq", split_axis=1, concat_axis=0, tiled=True),
    )
    row_count, col_count = local_q.shape
    head_count = col_count // HS
    query_heads = local_q.reshape(row_count, head_count, HS)

    def spots(first_row, total_rows):
        index_row = first_row + jnp.arange(total_rows, dtype=jnp.int32)
        owner = index_row // row_count
        within = index_row % row_count
        return (within // tok_rows * n_tensor + owner) * tok_rows + within % tok_rows

    query_usable = spots(tensor_index * row_count, row_count) < live_len
    initial = (
        jnp.full((row_count, head_count), MASKED_SCORE, jnp.float32),
        jnp.zeros((row_count, head_count), jnp.float32),
        jnp.zeros((row_count, head_count, HS), jnp.float32),
    )
    carried = initial
    first_row = jnp.int32(0)
    key_rows = lax.all_gather(local_k, "tensor", axis=0, tiled=True)
    value_rows = lax.all_gather(local_v, "tensor", axis=0, tiled=True)
    for offset in range(key_rows.shape[0] // row_count):
        row_peak, row_sum, accumulated = carried
        key_tile = key_rows[offset * row_count : (offset + 1) * row_count].reshape(
            row_count, head_count, HS
        )
        value_tile = value_rows[offset * row_count : (offset + 1) * row_count].reshape(
            row_count, head_count, HS
        )
        key_usable = spots(first_row + offset * row_count, row_count) < live_len
        scores = jnp.einsum(
            "qhd,khd->qhk", query_heads, key_tile, preferred_element_type=jnp.float32
        ) * HS ** (-0.5)
        scores = jnp.where(key_usable[None, None, :], scores, MASKED_SCORE)
        peak_new = jnp.maximum(row_peak, jnp.max(scores, axis=-1))
        exponent = jnp.where(key_usable[None, None, :], jnp.exp(scores - peak_new[..., None]), 0.0)
        rescale = jnp.exp(row_peak - peak_new)
        accumulated = accumulated * rescale[..., None] + jnp.einsum(
            "qhk,khd->qhd",
            exponent.astype(jnp.bfloat16),
            value_tile,
            preferred_element_type=jnp.float32,
        )
        carried = (peak_new, row_sum * rescale + jnp.sum(exponent, axis=-1), accumulated)
    row_peak, row_sum, accumulated = carried
    attended = accumulated / row_sum[..., None]
    mixed = jnp.where(query_usable[:, None], attended.reshape(row_count, col_count), 0.0).astype(
        jnp.bfloat16
    )
    restored = lax.all_to_all(mixed, "seq", split_axis=0, concat_axis=1, tiled=True)
    wide_weight = lax.all_gather(out_weight, "tensor", axis=1, tiled=True)
    summed = jnp.dot(
        restored,
        lax.all_gather(wide_weight, ("seq", "bucket"), axis=0, tiled=True),
        preferred_element_type=jnp.float32,
    )
    return summed.astype(jnp.bfloat16)[None]


def whole_kernel(
    axes, sizes, len_ref, q_ref, k_ref, v_ref, w_ref, out_ref,
    held, got, done, mixed, weight, part_out, part_in, own_part, load_sem, ready,
    qkv_send, qkv_recv, att_send, att_recv, up_send, down_send, line_recv,
    far_send, far_recv, near_send, near_recv, part_send, part_recv,
):
    n_seq, n_tensor, n_bucket = sizes
    s, t, b = lax.axis_index("seq"), lax.axis_index("tensor"), lax.axis_index("bucket")
    group = n_seq * n_tensor
    rows = q_ref.shape[1]
    width = q_ref.shape[2]
    heads = width // HS // group
    w_rows, w_cols = w_ref.shape

    def device(ds, dt, db):
        place = {"seq": ds, "tensor": dt, "bucket": db}
        return tuple(place[name] for name in axes)

    def remote(src, dst, send, recv, where):
        return pltpu.make_async_remote_copy(
            src_ref=src, dst_ref=dst, send_sem=send, recv_sem=recv,
            device_id=where, device_id_type=pl.DeviceIdType.MESH,
        )

    me = s * n_tensor + t
    streams = (q_ref, k_ref, v_ref)
    barrier = pltpu.get_barrier_semaphore()

    def spot(place):
        return pl.ds(pl.multiple_of(place * rows, rows), rows)

    def peer_of(e):
        return (s + e // n_tensor) % 2, (t + e % n_tensor) % n_tensor

    def source_of(e):
        return (s + e // n_tensor) % 2, (t + n_tensor - e % n_tensor) % n_tensor

    def drain(ref, sem):
        pltpu.make_async_copy(ref, ref, sem).wait()

    def qkv_copy(h, j, to, f):
        cols = pl.ds(pl.multiple_of(((to[0] * n_tensor + to[1]) * heads + h) * HS, HS), HS)
        return remote(
            held.at[j, :, cols],
            got.at[h, j, spot(me), :],
            qkv_send,
            qkv_recv.at[h, f if j == 0 else 2],
            device(to[0], to[1], b),
        )

    def start_stream(h, js, first, last, f):
        def body(d, carry):
            for j in js:
                qkv_copy(h, j, peer_of(f * n_tensor + d), f).start()
            return carry

        lax.fori_loop(first, last, body, 0)

    def side_rows(f):
        return pl.ds(pl.multiple_of((s + f) % 2 * n_tensor * rows, rows), n_tensor * rows)

    def arrive_kv(h):
        drain(got.at[h, pl.ds(1, 2)], qkv_recv.at[h, 2])

    def arrive_q(h, f):
        drain(got.at[h, 0, side_rows(f), :], qkv_recv.at[h, f])

    def start_across(h):
        start_stream(h, (1, 2, 0), 0, 1, 1)

    def start_kv_far(h, first=1, last=4):
        start_stream(h, (1, 2), first, last, 0)
        start_stream(h, (1, 2, 0), first, last, 1)

    def start_own(h):
        start_stream(h, (0,), 1, n_tensor, 0)

    def piece(row_block, col_block, c):
        return weight.at[
            c,
            pl.ds(pl.multiple_of(row_block * HS, HS), HS),
            pl.ds(pl.multiple_of(col_block * w_cols, w_cols), w_cols),
        ]

    def cut_of(p):
        return pl.ds(pl.multiple_of(p * w_cols, w_cols), w_cols)

    far, near = (b + 2) % 4, b + 1 - 2 * (b % 2)

    def up_copy(p, c):
        return remote(
            piece(b, p, c), piece(b, p, c), up_send, line_recv.at[p, c], device(s, t + 1, b)
        )

    def down_copy(p, c):
        return remote(
            piece(b, p, c), piece(b, p, c), down_send, line_recv.at[p, c], device(s, t - 1, b)
        )

    def far_copy(p, c, row_block):
        return remote(
            piece(row_block, p, c), piece(row_block, p, c), far_send, far_recv.at[p], device(s, t, far)
        )

    def near_copy(p, c, row_block):
        return remote(
            piece(row_block, p, c), piece(row_block, p, c), near_send, near_recv.at[p], device(s, t, near)
        )

    def spread(p, c):
        far_copy(p, c, b).start()
        near_copy(p, c, b).start()

    def relay_chunk(k, c):
        @pl.when(t >= k)
        def _():
            up_copy(t - k, c).wait_recv()

            @pl.when(t < n_tensor - 1)
            def _():
                up_copy(t - k, c).start()

            spread(t - k, c)

        @pl.when(t + k < n_tensor)
        def _():
            down_copy(t + k, c).wait_recv()

            @pl.when(t > 0)
            def _():
                down_copy(t + k, c).start()

            spread(t + k, c)

    def relay(k):
        for c in range(heads):
            relay_chunk(k, c)

    def weight_load(c):
        return pltpu.make_async_copy(w_ref.at[pl.ds(c * HS, HS), :], piece(b, t, c), load_sem.at[1])

    for c in range(heads):
        weight_load(c).start()

    def load(j):
        return pltpu.make_async_copy(streams[j].at[0], held.at[j], load_sem.at[0])

    def own_copy(h, j):
        cols = pl.ds(pl.multiple_of((me * heads + h) * HS, HS), HS)
        return pltpu.make_async_copy(
            streams[j].at[0, :, cols], got.at[h, j, spot(me), :], qkv_recv.at[h, 0 if j == 0 else 2]
        )

    def greet(semaphore, where):
        pl.semaphore_signal(semaphore, inc=1, device_id=where, device_id_type=pl.DeviceIdType.MESH)

    def greet_group(semaphore):
        greet(semaphore, device(1 - s, t, b))

        @pl.when(t > 0)
        def _():
            greet(semaphore, device(s, t - 1, b))

        @pl.when(t < n_tensor - 1)
        def _():
            greet(semaphore, device(s, t + 1, b))

    beside = 1 + (t > 0).astype(jnp.int32) + (t < n_tensor - 1).astype(jnp.int32)
    greet(barrier, device(s, t, far))
    greet(barrier, device(s, t, near))
    greet_group(barrier)
    for j in (1, 2, 0):
        load(j).start()
    for h in range(heads):
        for j in range(3):
            own_copy(h, j).start()
    pl.semaphore_wait(barrier, beside + 2)
    drain(weight.at[:, pl.ds(pl.multiple_of(b * HS, HS), HS), cut_of(t)], load_sem.at[1])

    for c in range(heads):
        @pl.when(t < n_tensor - 1)
        def _():
            up_copy(t, c).start()

        @pl.when(t > 0)
        def _():
            down_copy(t, c).start()

        spread(t, c)
    for k in range(3):
        greet_group(ready.at[k])
        pl.semaphore_wait(ready.at[k], beside)
    drain(held, load_sem.at[0])
    live = len_ref[0]

    upper = t // 2
    order = (t, 1 - t + 4 * upper, 2 - upper, 3 - 3 * upper)

    def forward(p):
        drain(weight.at[:, pl.ds(pl.multiple_of(far * HS, HS), HS), cut_of(p)], far_recv.at[p])
        for c in range(heads):
            near_copy(p, c, far).start()

    total = group * rows
    usable = lax.broadcasted_iota(jnp.int32, (1, total), 1) < live
    factor = HS ** (-0.5) * math.log2(math.e)

    def att_copy(h, f, target, source):
        cols = pl.ds(pl.multiple_of(source * HS, HS), HS)
        return remote(
            done.at[h, spot((s + f) % 2 * n_tensor + target), :], mixed.at[f, h, :, cols],
            att_send, att_recv.at[heads if f else h], device(s, target, b),
        )

    def attend_rows(h, query, own_token):
        scores = lax.dot_general(
            query, got[h, 1], (((1,), (1,)), ((), ())), preferred_element_type=jnp.float32
        )
        scores = jnp.where(usable, scores, MASKED_SCORE)
        peak = jnp.max(scores, axis=-1, keepdims=True)
        expo = jnp.exp2((scores - peak) * factor)
        denominator = jnp.sum(expo, axis=-1, keepdims=True)
        result = jnp.dot(expo.astype(jnp.bfloat16), got[h, 2], preferred_element_type=jnp.float32) / denominator
        return jnp.where(own_token < live, result, 0.0).astype(jnp.bfloat16)

    def attend(h, f):
        side = (s + f) % 2 * n_tensor
        row = lax.broadcasted_iota(jnp.int32, (rows, 1), 0)
        for step in range(0, n_tensor, 2):
            targets = [(t + step + i) % n_tensor for i in (1, 2)]
            spans = [spot(side + target) for target in targets]
            result = attend_rows(
                h,
                jnp.concatenate([got[h, 0, span, :] for span in spans], axis=0),
                jnp.concatenate([(side + target) * rows + row for target in targets], axis=0),
            )
            for i in range(2):
                d = step + i + 1
                if d < n_tensor:
                    done[h, spans[i], :] = result[i * rows : (i + 1) * rows]
                    att_copy(h, f, targets[i], t).start()
                else:
                    mixed[f, h, :, pl.ds(pl.multiple_of(t * HS, HS), HS)] = result[
                        i * rows : (i + 1) * rows
                    ]

    def back_far():
        drain(mixed.at[1, :, :, pl.ds(0, (n_tensor - 1) * HS)], att_recv.at[heads])

    def back_own(h):
        drain(mixed.at[0, h, :, pl.ds(0, (n_tensor - 1) * HS)], att_recv.at[h])

    def weight_sent():
        for n in range(1, n_tensor):
            @pl.when(t == n - 1)
            def _():
                drain(weight.at[:, pl.ds(0, HS), pl.ds(0, n * w_cols)], up_send)

            @pl.when(t == n_tensor - n)
            def _():
                drain(weight.at[:, pl.ds(0, HS), pl.ds(0, n * w_cols)], down_send)

        drain(weight.at[:, pl.ds(0, HS), :], far_send)
        drain(weight.at[:, pl.ds(0, 2 * HS), :], near_send)

    def part_copy(p):
        cut = cut_of(p)
        return remote(
            part_out.at[:, cut], part_in.at[:, cut], part_send, part_recv.at[p], device(1 - s, t, b)
        )

    def product(f, h, cut):
        return jnp.dot(mixed[f, h], weight[h, :, cut], preferred_element_type=jnp.float32)

    def own_product(h):
        for p in order:
            cut = cut_of(p)
            own_part[:, cut] = product(0, h, cut) if h == 0 else own_part[:, cut] + product(0, h, cut)

    def finish(p):
        cut = cut_of(p)
        mine = own_part[:, cut] + product(0, heads - 1, cut)
        part_copy(p).wait_recv()
        out_ref[0, :, cut] = (mine + part_in[:, cut].astype(jnp.float32)).astype(jnp.bfloat16)

    def project_far(k):
        p = order[k]
        cut = cut_of(p)
        drain(weight.at[:, pl.ds(0, 2 * HS), cut], near_recv.at[p])
        part_out[:, cut] = sum(product(1, h, cut) for h in range(heads)).astype(jnp.bfloat16)
        part_copy(p).start()


    for h in range(heads):
        start_across(h)

    relay(1)
    middle = ((t == 1) | (t == 2)).astype(jnp.int32)
    inner_first = jnp.where(t == 2, 2, 1)
    inner_last = inner_first + 2 * middle
    outer_first = jnp.where(t == 1, 3, 1)
    outer_last = jnp.where(t == 2, 2, 4)
    for h in range(heads):
        start_kv_far(h, inner_first, inner_last)
    forward(order[0])
    relay(2)
    for h in range(heads):
        start_kv_far(h, outer_first, outer_last)
    forward(order[1])
    relay(3)

    for h in range(heads):
        arrive_kv(h)
        arrive_q(h, 1)
        attend(h, 1)
        if h == 0:
            forward(order[2])
        if h == 1:
            forward(order[3])
            start_own(0)
    back_far()
    start_own(1)
    start_own(2)
    project_far(0)
    arrive_q(0, 0)
    attend(0, 0)
    project_far(1)
    arrive_q(1, 0)
    attend(1, 0)
    project_far(2)
    arrive_q(2, 0)
    attend(2, 0)
    project_far(3)
    weight_sent()
    back_own(0)
    own_product(0)
    back_own(1)
    own_product(1)
    back_own(2)
    for p in order:
        finish(p)
    drain(got.at[:, :, pl.ds(0, (group - 1) * rows), :], qkv_send)
    drain(done.at[:, pl.ds(0, n_seq * (n_tensor - 1) * rows), :], att_send)
    drain(part_out, part_send)


def fused(axes, sizes, queries, keys, values, lengths, out_weight):
    n_seq, n_tensor, n_bucket = sizes
    rows, width = queries.shape[1:]
    group = n_seq * n_tensor
    heads = width // HS // group
    total = group * rows
    anywhere = pl.BlockSpec(memory_space=pl.ANY)
    dma = pltpu.SemaphoreType.DMA
    return pl.pallas_call(
        functools.partial(whole_kernel, axes, sizes),
        out_shape=jax.ShapeDtypeStruct(queries.shape, queries.dtype),
        in_specs=[pl.BlockSpec(memory_space=pltpu.SMEM), anywhere, anywhere, anywhere, anywhere],
        out_specs=pl.BlockSpec(memory_space=pltpu.VMEM),
        scratch_shapes=[
            pltpu.VMEM((3, rows, width), jnp.bfloat16),
            pltpu.VMEM((heads, 3, total, HS), jnp.bfloat16),
            pltpu.VMEM((heads, total, HS), jnp.bfloat16),
            pltpu.VMEM((n_seq, heads, rows, n_tensor * HS), jnp.bfloat16),
            pltpu.VMEM((heads, n_bucket * HS, width), jnp.bfloat16),
            pltpu.VMEM((rows, width), jnp.bfloat16),
            pltpu.VMEM((rows, width), jnp.bfloat16),
            pltpu.VMEM((rows, width), jnp.float32),
            dma((2,)),
            pltpu.SemaphoreType.REGULAR((3,)),
            dma,
            dma((heads, 3)),
            dma,
            dma((heads + 1,)),
            dma,
            dma,
            dma((n_tensor, heads)),
            dma,
            dma((n_tensor,)),
            dma,
            dma((n_tensor,)),
            dma,
            dma((n_tensor,)),
        ],
        compiler_params=pltpu.CompilerParams(
            collective_id=0, has_side_effects=True, vmem_limit_bytes=32 * 1024 * 1024,
        ),
    )(lengths, *(pltpu.with_memory_space_constraint(x, pltpu.HBM) for x in (queries, keys, values, out_weight)))


def solution(mesh):
    in_specs = (
        P("bucket", ("seq", "tensor"), None),
        P("bucket", ("seq", "tensor"), None),
        P("bucket", ("seq", "tensor"), None),
        P("bucket"),
        P(("seq", "bucket"), "tensor"),
    )
    out_specs = P("bucket", ("seq", "tensor"), None)
    sizes = tuple(mesh.shape[name] for name in ("seq", "tensor", "bucket"))

    def step(queries, keys, values, lengths, out_weight):
        head_count = queries.shape[2] // HS
        fits = sizes[0] == 2 and sizes[1] == sizes[2] == 4 and head_count % (sizes[0] * sizes[1]) == 0
        if fits:
            return fused(mesh.axis_names, sizes, queries, keys, values, lengths, out_weight)
        return shards(queries, keys, values, lengths, out_weight)

    return jax.shard_map(step, mesh=mesh, in_specs=in_specs, out_specs=out_specs, check_vma=False)
```

```python
import functools
import math

import jax
import jax.numpy as jnp
from jax import lax
from jax.experimental import pallas as pl
from jax.experimental.pallas import tpu as pltpu
from jax.sharding import PartitionSpec as P

HS = 128


MASKED_SCORE = -1e30


def shards(queries, keys, values, lengths, out_weight):
    tok_rows = queries.shape[1]
    n_tensor = lax.axis_size("tensor")
    tensor_index = lax.axis_index("tensor")
    live_len = lengths[0]
    local_q, local_k, local_v = (
        lax.all_to_all(queries[0], "seq", split_axis=1, concat_axis=0, tiled=True),
        lax.all_to_all(keys[0], "seq", split_axis=1, concat_axis=0, tiled=True),
        lax.all_to_all(values[0], "seq", split_axis=1, concat_axis=0, tiled=True),
    )
    row_count, col_count = local_q.shape
    head_count = col_count // HS
    query_heads = local_q.reshape(row_count, head_count, HS)

    def spots(first_row, total_rows):
        index_row = first_row + jnp.arange(total_rows, dtype=jnp.int32)
        owner = index_row // row_count
        within = index_row % row_count
        return (within // tok_rows * n_tensor + owner) * tok_rows + within % tok_rows

    query_usable = spots(tensor_index * row_count, row_count) < live_len
    initial = (
        jnp.full((row_count, head_count), MASKED_SCORE, jnp.float32),
        jnp.zeros((row_count, head_count), jnp.float32),
        jnp.zeros((row_count, head_count, HS), jnp.float32),
    )
    carried = initial
    first_row = jnp.int32(0)
    key_rows = lax.all_gather(local_k, "tensor", axis=0, tiled=True)
    value_rows = lax.all_gather(local_v, "tensor", axis=0, tiled=True)
    for offset in range(key_rows.shape[0] // row_count):
        row_peak, row_sum, accumulated = carried
        key_tile = key_rows[offset * row_count : (offset + 1) * row_count].reshape(
            row_count, head_count, HS
        )
        value_tile = value_rows[offset * row_count : (offset + 1) * row_count].reshape(
            row_count, head_count, HS
        )
        key_usable = spots(first_row + offset * row_count, row_count) < live_len
        scores = jnp.einsum(
            "qhd,khd->qhk", query_heads, key_tile, preferred_element_type=jnp.float32
        ) * HS ** (-0.5)
        scores = jnp.where(key_usable[None, None, :], scores, MASKED_SCORE)
        peak_new = jnp.maximum(row_peak, jnp.max(scores, axis=-1))
        exponent = jnp.where(key_usable[None, None, :], jnp.exp(scores - peak_new[..., None]), 0.0)
        rescale = jnp.exp(row_peak - peak_new)
        accumulated = accumulated * rescale[..., None] + jnp.einsum(
            "qhk,khd->qhd",
            exponent.astype(jnp.bfloat16),
            value_tile,
            preferred_element_type=jnp.float32,
        )
        carried = (peak_new, row_sum * rescale + jnp.sum(exponent, axis=-1), accumulated)
    row_peak, row_sum, accumulated = carried
    attended = accumulated / row_sum[..., None]
    mixed = jnp.where(query_usable[:, None], attended.reshape(row_count, col_count), 0.0).astype(
        jnp.bfloat16
    )
    restored = lax.all_to_all(mixed, "seq", split_axis=0, concat_axis=1, tiled=True)
    wide_weight = lax.all_gather(out_weight, "tensor", axis=1, tiled=True)
    summed = jnp.dot(
        restored,
        lax.all_gather(wide_weight, ("seq", "bucket"), axis=0, tiled=True),
        preferred_element_type=jnp.float32,
    )
    return summed.astype(jnp.bfloat16)[None]


def whole_kernel(
    axes, sizes, len_ref, q_ref, k_ref, v_ref, w_ref, out_ref,
    held, got, done, mixed, weight, part_out, part_in, own_part, load_sem, ready,
    qkv_send, qkv_recv, att_send, att_recv, up_send, down_send, line_recv,
    far_send, far_recv, near_send, near_recv, part_send, part_recv,
):
    n_seq, n_tensor, n_bucket = sizes
    s, t, b = lax.axis_index("seq"), lax.axis_index("tensor"), lax.axis_index("bucket")
    group = n_seq * n_tensor
    rows = q_ref.shape[1]
    width = q_ref.shape[2]
    heads = width // HS // group
    w_rows, w_cols = w_ref.shape

    def device(ds, dt, db):
        place = {"seq": ds, "tensor": dt, "bucket": db}
        return tuple(place[name] for name in axes)

    def remote(src, dst, send, recv, where):
        return pltpu.make_async_remote_copy(
            src_ref=src, dst_ref=dst, send_sem=send, recv_sem=recv,
            device_id=where, device_id_type=pl.DeviceIdType.MESH,
        )

    me = s * n_tensor + t
    streams = (q_ref, k_ref, v_ref)
    barrier = pltpu.get_barrier_semaphore()

    def spot(place):
        return pl.ds(pl.multiple_of(place * rows, rows), rows)

    toward = 1 - 2 * (t // (n_tensor // 2))

    def along(i):
        return (t + toward * i + 2 * n_tensor) % n_tensor

    def drain(ref, sem):
        pltpu.make_async_copy(ref, ref, sem).wait()

    part_rows = rows // 2
    bands = ((0, 0, rows), (1, 0, part_rows), (1, part_rows, part_rows))

    def band_rows(g, place):
        f, first, count = bands[g]
        return pl.ds(pl.multiple_of(place * rows + first, part_rows), count)

    def send_copy(h, j, i, f, g):
        dt = along(i)
        ds = (s + f) % 2
        cols = pl.ds(pl.multiple_of(((ds * n_tensor + dt) * heads + h) * HS, HS), HS)
        first, count = (0, rows) if j else bands[g][1:]
        return remote(
            held.at[j, pl.ds(first, count), cols],
            got.at[h, j, pl.ds(pl.multiple_of(me * rows + first, part_rows), count), :],
            qkv_send,
            qkv_recv.at[h, 3 if j else g],
            device(ds, dt, b),
        )

    def start_kv(h, f, first, last):
        def body(i, carry):
            for j in (1, 2):
                send_copy(h, j, i, f, 0).start()
            return carry

        lax.fori_loop(first, last, body, 0)

    def start_q(h, g, first, last):
        def body(i, carry):
            send_copy(h, 0, i, bands[g][0], g).start()
            return carry

        lax.fori_loop(first, last, body, 0)

    def arrive_kv(h):
        drain(got.at[h, pl.ds(1, 2)], qkv_recv.at[h, 3])

    def arrive_q(h, g):
        drain(got.at[h, 0, pl.ds(0, n_tensor * bands[g][2]), :], qkv_recv.at[h, g])

    def piece(row_block, col_block, c):
        return weight.at[
            c,
            pl.ds(pl.multiple_of(row_block * HS, HS), HS),
            pl.ds(pl.multiple_of(col_block * w_cols, w_cols), w_cols),
        ]

    def cut_of(p):
        return pl.ds(pl.multiple_of(p * w_cols, w_cols), w_cols)

    far, near = (b + 2) % 4, b + 1 - 2 * (b % 2)

    def up_copy(p, c):
        return remote(
            piece(b, p, c), piece(b, p, c), up_send, line_recv.at[p, c], device(s, t + 1, b)
        )

    def down_copy(p, c):
        return remote(
            piece(b, p, c), piece(b, p, c), down_send, line_recv.at[p, c], device(s, t - 1, b)
        )

    def far_copy(p, c, row_block):
        return remote(
            piece(row_block, p, c), piece(row_block, p, c), far_send, far_recv.at[p], device(s, t, far)
        )

    def near_copy(p, c, row_block):
        return remote(
            piece(row_block, p, c), piece(row_block, p, c), near_send, near_recv.at[p], device(s, t, near)
        )

    def spread(p, c):
        far_copy(p, c, b).start()
        near_copy(p, c, b).start()

    def relay_chunk(k, c):
        @pl.when(t >= k)
        def _():
            up_copy(t - k, c).wait_recv()

            @pl.when(t < n_tensor - 1)
            def _():
                up_copy(t - k, c).start()

            spread(t - k, c)

        @pl.when(t + k < n_tensor)
        def _():
            down_copy(t + k, c).wait_recv()

            @pl.when(t > 0)
            def _():
                down_copy(t + k, c).start()

            spread(t + k, c)

    def relay(k):
        for c in range(heads):
            relay_chunk(k, c)

    def weight_load(c):
        return pltpu.make_async_copy(w_ref.at[pl.ds(c * HS, HS), :], piece(b, t, c), load_sem.at[1])

    for c in range(heads):
        weight_load(c).start()

    def load(j):
        return pltpu.make_async_copy(streams[j].at[0], held.at[j], load_sem.at[0])

    def own_copy(h, j):
        cols = pl.ds(pl.multiple_of((me * heads + h) * HS, HS), HS)
        return pltpu.make_async_copy(
            streams[j].at[0, :, cols], got.at[h, j, spot(me), :], qkv_recv.at[h, 3 if j else 0]
        )

    def greet(semaphore, where):
        pl.semaphore_signal(semaphore, inc=1, device_id=where, device_id_type=pl.DeviceIdType.MESH)

    def greet_group(semaphore):
        greet(semaphore, device(1 - s, t, b))

        @pl.when(t > 0)
        def _():
            greet(semaphore, device(s, t - 1, b))

        @pl.when(t < n_tensor - 1)
        def _():
            greet(semaphore, device(s, t + 1, b))

    beside = 1 + (t > 0).astype(jnp.int32) + (t < n_tensor - 1).astype(jnp.int32)
    greet(barrier, device(s, t, far))
    greet(barrier, device(s, t, near))
    greet_group(barrier)
    for j in (1, 2, 0):
        load(j).start()
    for h in range(heads):
        for j in range(3):
            own_copy(h, j).start()
    pl.semaphore_wait(barrier, beside + 2)
    drain(weight.at[:, pl.ds(pl.multiple_of(b * HS, HS), HS), cut_of(t)], load_sem.at[1])

    for c in range(heads):
        @pl.when(t < n_tensor - 1)
        def _():
            up_copy(t, c).start()

        @pl.when(t > 0)
        def _():
            down_copy(t, c).start()

        spread(t, c)
    for k in range(3):
        greet_group(ready.at[k])
        pl.semaphore_wait(ready.at[k], beside)
    drain(held, load_sem.at[0])
    live = len_ref[0]

    upper = t // 2
    order = (t, 1 - t + 4 * upper, 2 - upper, 3 - 3 * upper)

    def forward(p):
        drain(weight.at[:, pl.ds(pl.multiple_of(far * HS, HS), HS), cut_of(p)], far_recv.at[p])
        for c in range(heads):
            near_copy(p, c, far).start()

    total = group * rows
    usable = lax.broadcasted_iota(jnp.int32, (1, total), 1) < live
    factor = HS ** (-0.5) * math.log2(math.e)

    def att_copy(h, g, target):
        f, first, count = bands[g]
        return remote(
            done.at[h, band_rows(g, (s + f) % 2 * n_tensor + target), :],
            mixed.at[f, h, pl.ds(first, count), pl.ds(pl.multiple_of(t * HS, HS), HS)],
            att_send, att_recv.at[heads + g - 1 if f else h], device(s, target, b),
        )

    def attend_rows(h, query, own_token):
        scores = lax.dot_general(
            query, got[h, 1], (((1,), (1,)), ((), ())), preferred_element_type=jnp.float32
        )
        scores = jnp.where(usable, scores, MASKED_SCORE)
        peak = jnp.max(scores, axis=-1, keepdims=True)
        expo = jnp.exp2((scores - peak) * factor)
        denominator = jnp.sum(expo, axis=-1, keepdims=True)
        result = jnp.dot(expo.astype(jnp.bfloat16), got[h, 2], preferred_element_type=jnp.float32) / denominator
        return jnp.where(own_token < live, result, 0.0).astype(jnp.bfloat16)

    def attend(h, g):
        f, first, count = bands[g]
        side = (s + f) % 2 * n_tensor
        row = first + lax.broadcasted_iota(jnp.int32, (count, 1), 0)
        together = 2 * rows // count
        for step in range(0, n_tensor, together):
            targets = [along(step + i + 1) for i in range(together)]
            spans = [band_rows(g, side + target) for target in targets]
            result = attend_rows(
                h,
                jnp.concatenate([got[h, 0, span, :] for span in spans], axis=0),
                jnp.concatenate([(side + target) * rows + row for target in targets], axis=0),
            )
            for i in range(together):
                piece_rows = result[i * count : (i + 1) * count]
                if step + i + 1 < n_tensor:
                    done[h, spans[i], :] = piece_rows
                    att_copy(h, g, targets[i]).start()
                else:
                    mixed[f, h, pl.ds(first, count), pl.ds(pl.multiple_of(t * HS, HS), HS)] = piece_rows

    def back_far(g):
        drain(mixed.at[1, :, pl.ds(0, part_rows), pl.ds(0, (n_tensor - 1) * HS)], att_recv.at[heads + g - 1])

    def back_own(h):
        drain(mixed.at[0, h, :, pl.ds(0, (n_tensor - 1) * HS)], att_recv.at[h])

    def weight_sent():
        for n in range(1, n_tensor):
            @pl.when(t == n - 1)
            def _():
                drain(weight.at[:, pl.ds(0, HS), pl.ds(0, n * w_cols)], up_send)

            @pl.when(t == n_tensor - n)
            def _():
                drain(weight.at[:, pl.ds(0, HS), pl.ds(0, n * w_cols)], down_send)

        drain(weight.at[:, pl.ds(0, HS), :], far_send)
        drain(weight.at[:, pl.ds(0, 2 * HS), :], near_send)

    def part_copy(g, p):
        first, count = bands[g][1:]
        span, cut = pl.ds(first, count), cut_of(p)
        return remote(
            part_out.at[span, cut], part_in.at[span, cut], part_send, part_recv.at[p, g - 1], device(1 - s, t, b)
        )

    def product(g, h, cut):
        f, first, count = bands[g]
        return jnp.dot(
            mixed[f, h, first : first + count], weight[h, :, cut], preferred_element_type=jnp.float32
        )

    def own_product(h):
        for p in order:
            cut = cut_of(p)
            own_part[:, cut] = product(0, h, cut) if h == 0 else own_part[:, cut] + product(0, h, cut)

    def finish(p):
        cut = cut_of(p)
        mine = own_part[:, cut] + product(0, heads - 1, cut)
        for g in (1, 2):
            part_copy(g, p).wait_recv()
        out_ref[0, :, cut] = (mine + part_in[:, cut].astype(jnp.float32)).astype(jnp.bfloat16)

    def project_far(g, k):
        first, count = bands[g][1:]
        p = order[k]
        cut = cut_of(p)
        if g == 1:
            drain(weight.at[:, pl.ds(0, 2 * HS), cut], near_recv.at[p])
        part_out[first : first + count, cut] = sum(product(g, h, cut) for h in range(heads)).astype(jnp.bfloat16)
        part_copy(g, p).start()

    def start_far(h, first, last):
        start_kv(h, 0, first, last)
        start_kv(h, 1, first, last)
        start_q(h, 1, first, last)

    for h in range(heads):
        start_kv(h, 1, 0, 1)
        start_q(h, 1, 0, 1)
        start_q(h, 2, 0, 1)

    relay(1)
    inner = 1 + 2 * ((t == 1) | (t == 2)).astype(jnp.int32)
    for h in range(heads):
        start_far(h, 1, inner)
    forward(order[0])
    relay(2)
    for h in range(heads):
        start_far(h, inner, n_tensor)
    forward(order[1])
    relay(3)

    for h in range(heads):
        arrive_kv(h)
        arrive_q(h, 1)
        attend(h, 1)
        if h == 0:
            forward(order[2])
        if h == 1:
            forward(order[3])
            for k in range(heads):
                start_q(k, 2, 1, n_tensor)
    start_q(0, 0, 1, n_tensor)
    for h in range(heads):
        arrive_q(h, 2)
        attend(h, 2)
    start_q(1, 0, 1, n_tensor)
    start_q(2, 0, 1, n_tensor)
    back_far(1)
    for k in range(n_tensor):
        project_far(1, k)
    arrive_q(0, 0)
    attend(0, 0)
    back_far(2)
    for k in range(n_tensor):
        project_far(2, k)
    for h in range(1, heads):
        arrive_q(h, 0)
        attend(h, 0)
    weight_sent()
    back_own(0)
    own_product(0)
    back_own(1)
    own_product(1)
    back_own(2)
    for p in order:
        finish(p)
    drain(got.at[:, :, pl.ds(0, (group - 1) * rows), :], qkv_send)
    drain(done.at[:, pl.ds(0, n_seq * (n_tensor - 1) * rows), :], att_send)
    drain(part_out, part_send)


def fused(axes, sizes, queries, keys, values, lengths, out_weight):
    n_seq, n_tensor, n_bucket = sizes
    rows, width = queries.shape[1:]
    group = n_seq * n_tensor
    heads = width // HS // group
    total = group * rows
    anywhere = pl.BlockSpec(memory_space=pl.ANY)
    dma = pltpu.SemaphoreType.DMA
    return pl.pallas_call(
        functools.partial(whole_kernel, axes, sizes),
        out_shape=jax.ShapeDtypeStruct(queries.shape, queries.dtype),
        in_specs=[pl.BlockSpec(memory_space=pltpu.SMEM), anywhere, anywhere, anywhere, anywhere],
        out_specs=pl.BlockSpec(memory_space=pltpu.VMEM),
        scratch_shapes=[
            pltpu.VMEM((3, rows, width), jnp.bfloat16),
            pltpu.VMEM((heads, 3, total, HS), jnp.bfloat16),
            pltpu.VMEM((heads, total, HS), jnp.bfloat16),
            pltpu.VMEM((n_seq, heads, rows, n_tensor * HS), jnp.bfloat16),
            pltpu.VMEM((heads, n_bucket * HS, width), jnp.bfloat16),
            pltpu.VMEM((rows, width), jnp.bfloat16),
            pltpu.VMEM((rows, width), jnp.bfloat16),
            pltpu.VMEM((rows, width), jnp.float32),
            dma((2,)),
            pltpu.SemaphoreType.REGULAR((3,)),
            dma,
            dma((heads, 4)),
            dma,
            dma((heads + 2,)),
            dma,
            dma,
            dma((n_tensor, heads)),
            dma,
            dma((n_tensor,)),
            dma,
            dma((n_tensor,)),
            dma,
            dma((n_tensor, 2)),
        ],
        compiler_params=pltpu.CompilerParams(
            collective_id=0, has_side_effects=True, vmem_limit_bytes=32 * 1024 * 1024,
        ),
    )(lengths, *(pltpu.with_memory_space_constraint(x, pltpu.HBM) for x in (queries, keys, values, out_weight)))


def solution(mesh):
    in_specs = (
        P("bucket", ("seq", "tensor"), None),
        P("bucket", ("seq", "tensor"), None),
        P("bucket", ("seq", "tensor"), None),
        P("bucket"),
        P(("seq", "bucket"), "tensor"),
    )
    out_specs = P("bucket", ("seq", "tensor"), None)
    sizes = tuple(mesh.shape[name] for name in ("seq", "tensor", "bucket"))

    def step(queries, keys, values, lengths, out_weight):
        head_count = queries.shape[2] // HS
        fits = sizes[0] == 2 and sizes[1] == sizes[2] == 4 and head_count % (sizes[0] * sizes[1]) == 0
        if fits:
            return fused(mesh.axis_names, sizes, queries, keys, values, lengths, out_weight)
        return shards(queries, keys, values, lengths, out_weight)

    return jax.shard_map(step, mesh=mesh, in_specs=in_specs, out_specs=out_specs, check_vma=False)
```

```python
import functools
import math

import jax
import jax.numpy as jnp
from jax import lax
from jax.experimental import pallas as pl
from jax.experimental.pallas import tpu as pltpu
from jax.sharding import PartitionSpec as P

HS = 128


MASKED_SCORE = -1e30


def shards(queries, keys, values, lengths, out_weight):
    tok_rows = queries.shape[1]
    n_tensor = lax.axis_size("tensor")
    tensor_index = lax.axis_index("tensor")
    live_len = lengths[0]
    local_q, local_k, local_v = (
        lax.all_to_all(queries[0], "seq", split_axis=1, concat_axis=0, tiled=True),
        lax.all_to_all(keys[0], "seq", split_axis=1, concat_axis=0, tiled=True),
        lax.all_to_all(values[0], "seq", split_axis=1, concat_axis=0, tiled=True),
    )
    row_count, col_count = local_q.shape
    head_count = col_count // HS
    query_heads = local_q.reshape(row_count, head_count, HS)

    def spots(first_row, total_rows):
        index_row = first_row + jnp.arange(total_rows, dtype=jnp.int32)
        owner = index_row // row_count
        within = index_row % row_count
        return (within // tok_rows * n_tensor + owner) * tok_rows + within % tok_rows

    query_usable = spots(tensor_index * row_count, row_count) < live_len
    initial = (
        jnp.full((row_count, head_count), MASKED_SCORE, jnp.float32),
        jnp.zeros((row_count, head_count), jnp.float32),
        jnp.zeros((row_count, head_count, HS), jnp.float32),
    )
    carried = initial
    first_row = jnp.int32(0)
    key_rows = lax.all_gather(local_k, "tensor", axis=0, tiled=True)
    value_rows = lax.all_gather(local_v, "tensor", axis=0, tiled=True)
    for offset in range(key_rows.shape[0] // row_count):
        row_peak, row_sum, accumulated = carried
        key_tile = key_rows[offset * row_count : (offset + 1) * row_count].reshape(
            row_count, head_count, HS
        )
        value_tile = value_rows[offset * row_count : (offset + 1) * row_count].reshape(
            row_count, head_count, HS
        )
        key_usable = spots(first_row + offset * row_count, row_count) < live_len
        scores = jnp.einsum(
            "qhd,khd->qhk", query_heads, key_tile, preferred_element_type=jnp.float32
        ) * HS ** (-0.5)
        scores = jnp.where(key_usable[None, None, :], scores, MASKED_SCORE)
        peak_new = jnp.maximum(row_peak, jnp.max(scores, axis=-1))
        exponent = jnp.where(key_usable[None, None, :], jnp.exp(scores - peak_new[..., None]), 0.0)
        rescale = jnp.exp(row_peak - peak_new)
        accumulated = accumulated * rescale[..., None] + jnp.einsum(
            "qhk,khd->qhd",
            exponent.astype(jnp.bfloat16),
            value_tile,
            preferred_element_type=jnp.float32,
        )
        carried = (peak_new, row_sum * rescale + jnp.sum(exponent, axis=-1), accumulated)
    row_peak, row_sum, accumulated = carried
    attended = accumulated / row_sum[..., None]
    mixed = jnp.where(query_usable[:, None], attended.reshape(row_count, col_count), 0.0).astype(
        jnp.bfloat16
    )
    restored = lax.all_to_all(mixed, "seq", split_axis=0, concat_axis=1, tiled=True)
    wide_weight = lax.all_gather(out_weight, "tensor", axis=1, tiled=True)
    summed = jnp.dot(
        restored,
        lax.all_gather(wide_weight, ("seq", "bucket"), axis=0, tiled=True),
        preferred_element_type=jnp.float32,
    )
    return summed.astype(jnp.bfloat16)[None]


def whole_kernel(
    axes, sizes, len_ref, q_ref, k_ref, v_ref, w_ref, out_ref,
    held, got, done, mixed, weight, part_out, part_in, own_part, load_sem, ready,
    qkv_send, qkv_recv, att_send, att_recv, up_send, down_send, line_recv,
    far_send, far_recv, near_send, near_recv, part_send, part_recv,
):
    n_seq, n_tensor, n_bucket = sizes
    s, t, b = lax.axis_index("seq"), lax.axis_index("tensor"), lax.axis_index("bucket")
    group = n_seq * n_tensor
    rows = q_ref.shape[1]
    width = q_ref.shape[2]
    heads = width // HS // group
    w_rows, w_cols = w_ref.shape

    def device(ds, dt, db):
        place = {"seq": ds, "tensor": dt, "bucket": db}
        return tuple(place[name] for name in axes)

    def remote(src, dst, send, recv, where):
        return pltpu.make_async_remote_copy(
            src_ref=src, dst_ref=dst, send_sem=send, recv_sem=recv,
            device_id=where, device_id_type=pl.DeviceIdType.MESH,
        )

    me = s * n_tensor + t
    streams = (q_ref, k_ref, v_ref)
    barrier = pltpu.get_barrier_semaphore()

    def spot(place):
        return pl.ds(pl.multiple_of(place * rows, rows), rows)

    toward = 1 - 2 * (t // (n_tensor // 2))

    def along(i):
        return (t + toward * i + 2 * n_tensor) % n_tensor

    def drain(ref, sem):
        pltpu.make_async_copy(ref, ref, sem).wait()

    part_rows = rows // 2
    bands = ((0, 0, rows), (1, 0, part_rows), (1, part_rows, part_rows))

    def band_rows(g, place):
        f, first, count = bands[g]
        return pl.ds(pl.multiple_of(place * rows + first, part_rows), count)

    def send_copy(h, j, i, f, g):
        dt = along(i)
        ds = (s + f) % 2
        cols = pl.ds(pl.multiple_of(((ds * n_tensor + dt) * heads + h) * HS, HS), HS)
        first, count = (0, rows) if j else bands[g][1:]
        return remote(
            held.at[j, pl.ds(first, count), cols],
            got.at[h, j, pl.ds(pl.multiple_of(me * rows + first, part_rows), count), :],
            qkv_send,
            qkv_recv.at[h, 3 if j else g],
            device(ds, dt, b),
        )

    def start_kv(h, f, first, last):
        def body(i, carry):
            for j in (1, 2):
                send_copy(h, j, i, f, 0).start()
            return carry

        lax.fori_loop(first, last, body, 0)

    def start_q(h, g, first, last):
        def body(i, carry):
            send_copy(h, 0, i, bands[g][0], g).start()
            return carry

        lax.fori_loop(first, last, body, 0)

    def arrive_kv(h):
        drain(got.at[h, pl.ds(1, 2)], qkv_recv.at[h, 3])

    def arrive_q(h, g):
        drain(got.at[h, 0, pl.ds(0, n_tensor * bands[g][2]), :], qkv_recv.at[h, g])

    def piece(row_block, col_block, c):
        return weight.at[
            c,
            pl.ds(pl.multiple_of(row_block * HS, HS), HS),
            pl.ds(pl.multiple_of(col_block * w_cols, w_cols), w_cols),
        ]

    def cut_of(p):
        return pl.ds(pl.multiple_of(p * w_cols, w_cols), w_cols)

    far, near = (b + 2) % 4, b + 1 - 2 * (b % 2)

    def up_copy(p, c):
        return remote(
            piece(b, p, c), piece(b, p, c), up_send, line_recv.at[p, c], device(s, t + 1, b)
        )

    def down_copy(p, c):
        return remote(
            piece(b, p, c), piece(b, p, c), down_send, line_recv.at[p, c], device(s, t - 1, b)
        )

    def far_copy(p, c, row_block):
        return remote(
            piece(row_block, p, c), piece(row_block, p, c), far_send, far_recv.at[p], device(s, t, far)
        )

    def near_copy(p, c, row_block):
        return remote(
            piece(row_block, p, c), piece(row_block, p, c), near_send, near_recv.at[p], device(s, t, near)
        )

    def spread(p, c):
        far_copy(p, c, b).start()
        near_copy(p, c, b).start()

    def relay_chunk(k, c):
        @pl.when(t >= k)
        def _():
            up_copy(t - k, c).wait_recv()

            @pl.when(t < n_tensor - 1)
            def _():
                up_copy(t - k, c).start()

            spread(t - k, c)

        @pl.when(t + k < n_tensor)
        def _():
            down_copy(t + k, c).wait_recv()

            @pl.when(t > 0)
            def _():
                down_copy(t + k, c).start()

            spread(t + k, c)

    def relay(k):
        for c in range(heads):
            relay_chunk(k, c)

    def weight_load(c):
        return pltpu.make_async_copy(w_ref.at[pl.ds(c * HS, HS), :], piece(b, t, c), load_sem.at[1])

    def load(j):
        return pltpu.make_async_copy(streams[j].at[0], held.at[j], load_sem.at[0])

    def own_copy(h, j):
        cols = pl.ds(pl.multiple_of((me * heads + h) * HS, HS), HS)
        return pltpu.make_async_copy(
            streams[j].at[0, :, cols], got.at[h, j, spot(me), :], qkv_recv.at[h, 3 if j else 0]
        )

    def greet(semaphore, where):
        pl.semaphore_signal(semaphore, inc=1, device_id=where, device_id_type=pl.DeviceIdType.MESH)

    def greet_group(semaphore):
        greet(semaphore, device(1 - s, t, b))

        @pl.when(t > 0)
        def _():
            greet(semaphore, device(s, t - 1, b))

        @pl.when(t < n_tensor - 1)
        def _():
            greet(semaphore, device(s, t + 1, b))

    beside = 1 + (t > 0).astype(jnp.int32) + (t < n_tensor - 1).astype(jnp.int32)
    greet_group(barrier)
    greet(barrier, device(s, t, far))
    greet(barrier, device(s, t, near))
    for c in range(heads):
        weight_load(c).start()
    pl.semaphore_wait(barrier, beside + 2)
    drain(weight.at[:, pl.ds(pl.multiple_of(b * HS, HS), HS), cut_of(t)], load_sem.at[1])

    for c in range(heads):
        @pl.when(t < n_tensor - 1)
        def _():
            up_copy(t, c).start()

        @pl.when(t > 0)
        def _():
            down_copy(t, c).start()

        spread(t, c)
    for j in (1, 2, 0):
        load(j).start()
    for h in range(heads):
        for j in range(3):
            own_copy(h, j).start()
    for k in range(3):
        greet_group(ready.at[k])
        pl.semaphore_wait(ready.at[k], beside)
    drain(held, load_sem.at[0])
    live = len_ref[0]

    upper = t // 2
    order = (t, 1 - t + 4 * upper, 2 - upper, 3 - 3 * upper)

    def forward(p):
        drain(weight.at[:, pl.ds(pl.multiple_of(far * HS, HS), HS), cut_of(p)], far_recv.at[p])
        for c in range(heads):
            near_copy(p, c, far).start()

    total = group * rows
    usable = lax.broadcasted_iota(jnp.int32, (1, total), 1) < live
    factor = HS ** (-0.5) * math.log2(math.e)

    def att_copy(h, g, target):
        f, first, count = bands[g]
        return remote(
            done.at[h, band_rows(g, (s + f) % 2 * n_tensor + target), :],
            mixed.at[f, h, pl.ds(first, count), pl.ds(pl.multiple_of(t * HS, HS), HS)],
            att_send, att_recv.at[heads + g - 1 if f else h], device(s, target, b),
        )

    def attend_rows(h, query, own_token):
        scores = lax.dot_general(
            query, got[h, 1], (((1,), (1,)), ((), ())), preferred_element_type=jnp.float32
        )
        scores = jnp.where(usable, scores, MASKED_SCORE)
        peak = jnp.max(scores, axis=-1, keepdims=True)
        expo = jnp.exp2((scores - peak) * factor)
        denominator = jnp.sum(expo, axis=-1, keepdims=True)
        result = jnp.dot(expo.astype(jnp.bfloat16), got[h, 2], preferred_element_type=jnp.float32) / denominator
        return jnp.where(own_token < live, result, 0.0).astype(jnp.bfloat16)

    def attend(h, g):
        f, first, count = bands[g]
        side = (s + f) % 2 * n_tensor
        row = first + lax.broadcasted_iota(jnp.int32, (count, 1), 0)
        together = 2 * rows // count
        for step in range(0, n_tensor, together):
            targets = [along(step + i + 1 if g or step + i + 1 == n_tensor else n_tensor - 1 - step - i) for i in range(together)]
            spans = [band_rows(g, side + target) for target in targets]
            result = attend_rows(
                h,
                jnp.concatenate([got[h, 0, span, :] for span in spans], axis=0),
                jnp.concatenate([(side + target) * rows + row for target in targets], axis=0),
            )
            for i in range(together):
                piece_rows = result[i * count : (i + 1) * count]
                if step + i + 1 < n_tensor:
                    done[h, spans[i], :] = piece_rows
                    att_copy(h, g, targets[i]).start()
                else:
                    mixed[f, h, pl.ds(first, count), pl.ds(pl.multiple_of(t * HS, HS), HS)] = piece_rows

    def back_far(g):
        drain(mixed.at[1, :, pl.ds(0, part_rows), pl.ds(0, (n_tensor - 1) * HS)], att_recv.at[heads + g - 1])

    def back_own(h):
        drain(mixed.at[0, h, :, pl.ds(0, (n_tensor - 1) * HS)], att_recv.at[h])

    def weight_sent():
        for n in range(1, n_tensor):
            @pl.when(t == n - 1)
            def _():
                drain(weight.at[:, pl.ds(0, HS), pl.ds(0, n * w_cols)], up_send)

            @pl.when(t == n_tensor - n)
            def _():
                drain(weight.at[:, pl.ds(0, HS), pl.ds(0, n * w_cols)], down_send)

        drain(weight.at[:, pl.ds(0, HS), :], far_send)
        drain(weight.at[:, pl.ds(0, 2 * HS), :], near_send)

    def part_copy(g, p):
        first, count = bands[g][1:]
        span, cut = pl.ds(first, count), cut_of(p)
        return remote(
            part_out.at[span, cut], part_in.at[span, cut], part_send, part_recv.at[p, g - 1], device(1 - s, t, b)
        )

    def product(g, h, cut):
        f, first, count = bands[g]
        return jnp.dot(
            mixed[f, h, first : first + count], weight[h, :, cut], preferred_element_type=jnp.float32
        )

    def own_product(h):
        for p in order:
            cut = cut_of(p)
            own_part[:, cut] = product(0, h, cut) if h == 0 else own_part[:, cut] + product(0, h, cut)

    def merge(p):
        cut = cut_of(p)
        for g in (1, 2):
            part_copy(g, p).wait_recv()
        own_part[:, cut] = own_part[:, cut] + part_in[:, cut].astype(jnp.float32)

    def finish(first, last):
        cut = slice(first * w_cols, last * w_cols)
        out_ref[0, :, cut] = (own_part[:, cut] + product(0, heads - 1, cut)).astype(jnp.bfloat16)

    def project_far(g, k):
        first, count = bands[g][1:]
        p = order[k]
        cut = cut_of(p)
        if g == 1:
            drain(weight.at[:, pl.ds(0, 2 * HS), cut], near_recv.at[p])
        part_out[first : first + count, cut] = sum(product(g, h, cut) for h in range(heads)).astype(jnp.bfloat16)
        part_copy(g, p).start()

    def start_far(h, first, last):
        start_kv(h, 0, first, last)
        start_kv(h, 1, first, last)
        start_q(h, 1, first, last)

    for h in range(heads):
        start_kv(h, 1, 0, 1)
        start_q(h, 1, 0, 1)
        start_q(h, 2, 0, 1)

    relay(1)
    inner = 1 + 2 * ((t == 1) | (t == 2)).astype(jnp.int32)
    for h in range(heads):
        start_far(h, 1, inner)
    forward(order[0])
    relay(2)
    for h in range(heads):
        start_far(h, inner, n_tensor)
    forward(order[1])
    relay(3)

    for h in range(heads):
        arrive_kv(h)
        arrive_q(h, 1)
        attend(h, 1)
        if h == 0:
            forward(order[2])
        if h == 1:
            forward(order[3])
            for k in range(heads):
                start_q(k, 2, 1, n_tensor)
    start_q(0, 0, 1, n_tensor)
    for h in range(heads):
        arrive_q(h, 2)
        attend(h, 2)
    start_q(1, 0, 1, n_tensor)
    start_q(2, 0, 1, n_tensor)
    back_far(1)
    for k in range(n_tensor):
        project_far(1, k)
    arrive_q(0, 0)
    attend(0, 0)
    back_far(2)
    for k in range(n_tensor):
        project_far(2, k)
    for h in range(1, heads):
        arrive_q(h, 0)
        attend(h, 0)
    weight_sent()
    back_own(0)
    own_product(0)
    back_own(1)
    own_product(1)
    for p in order:
        merge(p)
    back_own(2)
    finish(0, 1)
    finish(1, 2)
    finish(2, 3)
    finish(3, 4)
    drain(got.at[:, :, pl.ds(0, (group - 1) * rows), :], qkv_send)
    drain(done.at[:, pl.ds(0, n_seq * (n_tensor - 1) * rows), :], att_send)
    drain(part_out, part_send)


def fused(axes, sizes, queries, keys, values, lengths, out_weight):
    n_seq, n_tensor, n_bucket = sizes
    rows, width = queries.shape[1:]
    group = n_seq * n_tensor
    heads = width // HS // group
    total = group * rows
    anywhere = pl.BlockSpec(memory_space=pl.ANY)
    dma = pltpu.SemaphoreType.DMA
    return pl.pallas_call(
        functools.partial(whole_kernel, axes, sizes),
        out_shape=jax.ShapeDtypeStruct(queries.shape, queries.dtype),
        in_specs=[pl.BlockSpec(memory_space=pltpu.SMEM), anywhere, anywhere, anywhere, anywhere],
        out_specs=pl.BlockSpec(memory_space=pltpu.VMEM),
        scratch_shapes=[
            pltpu.VMEM((3, rows, width), jnp.bfloat16),
            pltpu.VMEM((heads, 3, total, HS), jnp.bfloat16),
            pltpu.VMEM((heads, total, HS), jnp.bfloat16),
            pltpu.VMEM((n_seq, heads, rows, n_tensor * HS), jnp.bfloat16),
            pltpu.VMEM((heads, n_bucket * HS, width), jnp.bfloat16),
            pltpu.VMEM((rows, width), jnp.bfloat16),
            pltpu.VMEM((rows, width), jnp.bfloat16),
            pltpu.VMEM((rows, width), jnp.float32),
            dma((2,)),
            pltpu.SemaphoreType.REGULAR((3,)),
            dma,
            dma((heads, 4)),
            dma,
            dma((heads + 2,)),
            dma,
            dma,
            dma((n_tensor, heads)),
            dma,
            dma((n_tensor,)),
            dma,
            dma((n_tensor,)),
            dma,
            dma((n_tensor, 2)),
        ],
        compiler_params=pltpu.CompilerParams(
            collective_id=0, has_side_effects=True, vmem_limit_bytes=32 * 1024 * 1024,
        ),
    )(lengths, *(pltpu.with_memory_space_constraint(x, pltpu.HBM) for x in (queries, keys, values, out_weight)))


def solution(mesh):
    in_specs = (
        P("bucket", ("seq", "tensor"), None),
        P("bucket", ("seq", "tensor"), None),
        P("bucket", ("seq", "tensor"), None),
        P("bucket"),
        P(("seq", "bucket"), "tensor"),
    )
    out_specs = P("bucket", ("seq", "tensor"), None)
    sizes = tuple(mesh.shape[name] for name in ("seq", "tensor", "bucket"))

    def step(queries, keys, values, lengths, out_weight):
        head_count = queries.shape[2] // HS
        fits = sizes[0] == 2 and sizes[1] == sizes[2] == 4 and head_count % (sizes[0] * sizes[1]) == 0
        if fits:
            return fused(mesh.axis_names, sizes, queries, keys, values, lengths, out_weight)
        return shards(queries, keys, values, lengths, out_weight)

    return jax.shard_map(step, mesh=mesh, in_specs=in_specs, out_specs=out_specs, check_vma=False)
```

```python
import functools
import math

import jax
import jax.numpy as jnp
from jax import lax
from jax.experimental import pallas as pl
from jax.experimental.pallas import tpu as pltpu
from jax.sharding import PartitionSpec as P

HS = 128


MASKED_SCORE = -1e30


def shards(queries, keys, values, lengths, out_weight):
    tok_rows = queries.shape[1]
    n_tensor = lax.axis_size("tensor")
    tensor_index = lax.axis_index("tensor")
    live_len = lengths[0]
    local_q, local_k, local_v = (
        lax.all_to_all(queries[0], "seq", split_axis=1, concat_axis=0, tiled=True),
        lax.all_to_all(keys[0], "seq", split_axis=1, concat_axis=0, tiled=True),
        lax.all_to_all(values[0], "seq", split_axis=1, concat_axis=0, tiled=True),
    )
    row_count, col_count = local_q.shape
    head_count = col_count // HS
    query_heads = local_q.reshape(row_count, head_count, HS)

    def spots(first_row, total_rows):
        index_row = first_row + jnp.arange(total_rows, dtype=jnp.int32)
        owner = index_row // row_count
        within = index_row % row_count
        return (within // tok_rows * n_tensor + owner) * tok_rows + within % tok_rows

    query_usable = spots(tensor_index * row_count, row_count) < live_len
    initial = (
        jnp.full((row_count, head_count), MASKED_SCORE, jnp.float32),
        jnp.zeros((row_count, head_count), jnp.float32),
        jnp.zeros((row_count, head_count, HS), jnp.float32),
    )
    carried = initial
    first_row = jnp.int32(0)
    key_rows = lax.all_gather(local_k, "tensor", axis=0, tiled=True)
    value_rows = lax.all_gather(local_v, "tensor", axis=0, tiled=True)
    for offset in range(key_rows.shape[0] // row_count):
        row_peak, row_sum, accumulated = carried
        key_tile = key_rows[offset * row_count : (offset + 1) * row_count].reshape(
            row_count, head_count, HS
        )
        value_tile = value_rows[offset * row_count : (offset + 1) * row_count].reshape(
            row_count, head_count, HS
        )
        key_usable = spots(first_row + offset * row_count, row_count) < live_len
        scores = jnp.einsum(
            "qhd,khd->qhk", query_heads, key_tile, preferred_element_type=jnp.float32
        ) * HS ** (-0.5)
        scores = jnp.where(key_usable[None, None, :], scores, MASKED_SCORE)
        peak_new = jnp.maximum(row_peak, jnp.max(scores, axis=-1))
        exponent = jnp.where(key_usable[None, None, :], jnp.exp(scores - peak_new[..., None]), 0.0)
        rescale = jnp.exp(row_peak - peak_new)
        accumulated = accumulated * rescale[..., None] + jnp.einsum(
            "qhk,khd->qhd",
            exponent.astype(jnp.bfloat16),
            value_tile,
            preferred_element_type=jnp.float32,
        )
        carried = (peak_new, row_sum * rescale + jnp.sum(exponent, axis=-1), accumulated)
    row_peak, row_sum, accumulated = carried
    attended = accumulated / row_sum[..., None]
    mixed = jnp.where(query_usable[:, None], attended.reshape(row_count, col_count), 0.0).astype(
        jnp.bfloat16
    )
    restored = lax.all_to_all(mixed, "seq", split_axis=0, concat_axis=1, tiled=True)
    wide_weight = lax.all_gather(out_weight, "tensor", axis=1, tiled=True)
    summed = jnp.dot(
        restored,
        lax.all_gather(wide_weight, ("seq", "bucket"), axis=0, tiled=True),
        preferred_element_type=jnp.float32,
    )
    return summed.astype(jnp.bfloat16)[None]


def whole_kernel(
    axes, sizes, len_ref, q_ref, k_ref, v_ref, w_ref, out_ref,
    held, got, done, mixed, weight, part_out, part_in, own_part, load_sem, ready,
    qkv_send, qkv_recv, att_send, att_recv, up_send, down_send, line_recv,
    far_send, far_recv, near_send, near_recv, part_send, part_recv,
):
    n_seq, n_tensor, n_bucket = sizes
    s, t, b = lax.axis_index("seq"), lax.axis_index("tensor"), lax.axis_index("bucket")
    group = n_seq * n_tensor
    rows = q_ref.shape[1]
    width = q_ref.shape[2]
    heads = width // HS // group
    w_rows, w_cols = w_ref.shape

    def device(ds, dt, db):
        place = {"seq": ds, "tensor": dt, "bucket": db}
        return tuple(place[name] for name in axes)

    def remote(src, dst, send, recv, where):
        return pltpu.make_async_remote_copy(
            src_ref=src, dst_ref=dst, send_sem=send, recv_sem=recv,
            device_id=where, device_id_type=pl.DeviceIdType.MESH,
        )

    me = s * n_tensor + t
    streams = (q_ref, k_ref, v_ref)
    barrier = pltpu.get_barrier_semaphore()

    def spot(place):
        return pl.ds(pl.multiple_of(place * rows, rows), rows)

    toward = 1 - 2 * (t // (n_tensor // 2))

    def along(i):
        return (t + toward * i + 2 * n_tensor) % n_tensor

    def drain(ref, sem):
        pltpu.make_async_copy(ref, ref, sem).wait()

    part_rows = rows // 2
    bands = ((0, 0, rows), (1, 0, part_rows), (1, part_rows, part_rows))

    def band_rows(g, place):
        f, first, count = bands[g]
        return pl.ds(pl.multiple_of(place * rows + first, part_rows), count)

    def send_copy(h, j, i, f, g):
        dt = along(i)
        ds = (s + f) % 2
        cols = pl.ds(pl.multiple_of(((ds * n_tensor + dt) * heads + h) * HS, HS), HS)
        first, count = (0, rows) if j else bands[g][1:]
        return remote(
            held.at[j, pl.ds(first, count), cols],
            got.at[h, j, pl.ds(pl.multiple_of(me * rows + first, part_rows), count), :],
            qkv_send,
            qkv_recv.at[h, 1 if j else g],
            device(ds, dt, b),
        )

    def start_kv(h, f, first, last):
        def body(i, carry):
            for j in (1, 2):
                send_copy(h, j, i, f, 0).start()
            return carry

        lax.fori_loop(first, last, body, 0)

    def start_q(h, g, first, last):
        def body(i, carry):
            send_copy(h, 0, i, bands[g][0], g).start()
            return carry

        lax.fori_loop(first, last, body, 0)

    def arrive_kv(h):
        drain(got.at[h, :, pl.ds(0, (2 * group * rows + n_tensor * part_rows) // 3), :], qkv_recv.at[h, 1])

    def arrive_q(h, g):
        drain(got.at[h, 0, pl.ds(0, n_tensor * bands[g][2]), :], qkv_recv.at[h, g])

    def piece(row_block, col_block, c):
        return weight.at[
            c,
            pl.ds(pl.multiple_of(row_block * HS, HS), HS),
            pl.ds(pl.multiple_of(col_block * w_cols, w_cols), w_cols),
        ]

    def cut_of(p):
        return pl.ds(pl.multiple_of(p * w_cols, w_cols), w_cols)

    far, near = (b + 2) % 4, b + 1 - 2 * (b % 2)

    def up_copy(p, c):
        return remote(
            piece(b, p, c), piece(b, p, c), up_send, line_recv.at[p, c], device(s, t + 1, b)
        )

    def down_copy(p, c):
        return remote(
            piece(b, p, c), piece(b, p, c), down_send, line_recv.at[p, c], device(s, t - 1, b)
        )

    def far_copy(p, c, row_block):
        return remote(
            piece(row_block, p, c), piece(row_block, p, c), far_send, far_recv.at[p], device(s, t, far)
        )

    def near_copy(p, c, row_block):
        return remote(
            piece(row_block, p, c), piece(row_block, p, c), near_send, near_recv.at[p], device(s, t, near)
        )

    def spread(p, c):
        far_copy(p, c, b).start()
        near_copy(p, c, b).start()

    def relay_chunk(k, c):
        @pl.when(t >= k)
        def _():
            up_copy(t - k, c).wait_recv()

            @pl.when(t < n_tensor - 1)
            def _():
                up_copy(t - k, c).start()

            spread(t - k, c)

        @pl.when(t + k < n_tensor)
        def _():
            down_copy(t + k, c).wait_recv()

            @pl.when(t > 0)
            def _():
                down_copy(t + k, c).start()

            spread(t + k, c)

    def relay(k):
        for c in range(heads):
            relay_chunk(k, c)

    def weight_load(c):
        return pltpu.make_async_copy(w_ref.at[pl.ds(c * HS, HS), :], piece(b, t, c), load_sem.at[1])

    def load(j):
        return pltpu.make_async_copy(streams[j].at[0], held.at[j], load_sem.at[0])

    def own_copy(h, j):
        cols = pl.ds(pl.multiple_of((me * heads + h) * HS, HS), HS)
        return pltpu.make_async_copy(
            streams[j].at[0, :, cols], got.at[h, j, spot(me), :], qkv_recv.at[h, 1 if j else 0]
        )

    def greet(semaphore, where):
        pl.semaphore_signal(semaphore, inc=1, device_id=where, device_id_type=pl.DeviceIdType.MESH)

    def greet_group(semaphore):
        greet(semaphore, device(1 - s, t, b))

        @pl.when(t > 0)
        def _():
            greet(semaphore, device(s, t - 1, b))

        @pl.when(t < n_tensor - 1)
        def _():
            greet(semaphore, device(s, t + 1, b))

    beside = 1 + (t > 0).astype(jnp.int32) + (t < n_tensor - 1).astype(jnp.int32)
    greet_group(barrier)
    greet(barrier, device(s, t, far))
    greet(barrier, device(s, t, near))
    for c in range(heads):
        weight_load(c).start()
    pl.semaphore_wait(barrier, beside + 2)
    drain(weight.at[:, pl.ds(pl.multiple_of(b * HS, HS), HS), cut_of(t)], load_sem.at[1])

    for c in range(heads):
        @pl.when(t < n_tensor - 1)
        def _():
            up_copy(t, c).start()

        @pl.when(t > 0)
        def _():
            down_copy(t, c).start()

        spread(t, c)
    for j in (1, 2, 0):
        load(j).start()
    for h in range(heads):
        for j in range(3):
            own_copy(h, j).start()
    for k in range(3):
        greet_group(ready.at[k])
        pl.semaphore_wait(ready.at[k], beside)
    drain(held, load_sem.at[0])
    live = len_ref[0]

    upper = t // 2
    order = (t, 1 - t + 4 * upper, 2 - upper, 3 - 3 * upper)

    def forward(p):
        drain(weight.at[:, pl.ds(pl.multiple_of(far * HS, HS), HS), cut_of(p)], far_recv.at[p])
        for c in range(heads):
            near_copy(p, c, far).start()

    total = group * rows
    usable = lax.broadcasted_iota(jnp.int32, (1, total), 1) < live
    factor = HS ** (-0.5) * math.log2(math.e)

    def att_copy(h, g, target):
        f, first, count = bands[g]
        return remote(
            done.at[h, band_rows(g, (s + f) % 2 * n_tensor + target), :],
            mixed.at[f, h, pl.ds(first, count), pl.ds(pl.multiple_of(t * HS, HS), HS)],
            att_send, att_recv.at[heads + g - 1 if f else h], device(s, target, b),
        )

    def attend_rows(h, query, own_token):
        scores = lax.dot_general(
            query, got[h, 1], (((1,), (1,)), ((), ())), preferred_element_type=jnp.float32
        )
        scores = jnp.where(usable, scores, MASKED_SCORE)
        peak = jnp.max(scores, axis=-1, keepdims=True)
        expo = jnp.exp2((scores - peak) * factor)
        denominator = jnp.sum(expo, axis=-1, keepdims=True)
        result = jnp.dot(expo.astype(jnp.bfloat16), got[h, 2], preferred_element_type=jnp.float32) / denominator
        return jnp.where(own_token < live, result, 0.0).astype(jnp.bfloat16)

    def attend(h, g):
        f, first, count = bands[g]
        side = (s + f) % 2 * n_tensor
        row = first + lax.broadcasted_iota(jnp.int32, (count, 1), 0)
        together = 2 * rows // count
        for step in range(0, n_tensor, together):
            targets = [along(step + i + 1 if g or step + i + 1 == n_tensor else n_tensor - 1 - step - i) for i in range(together)]
            spans = [band_rows(g, side + target) for target in targets]
            result = attend_rows(
                h,
                jnp.concatenate([got[h, 0, span, :] for span in spans], axis=0),
                jnp.concatenate([(side + target) * rows + row for target in targets], axis=0),
            )
            for i in range(together):
                piece_rows = result[i * count : (i + 1) * count]
                if step + i + 1 < n_tensor:
                    done[h, spans[i], :] = piece_rows
                    att_copy(h, g, targets[i]).start()
                else:
                    mixed[f, h, pl.ds(first, count), pl.ds(pl.multiple_of(t * HS, HS), HS)] = piece_rows

    def back_far(g):
        drain(mixed.at[1, :, pl.ds(0, part_rows), pl.ds(0, (n_tensor - 1) * HS)], att_recv.at[heads + g - 1])

    def back_own(h):
        drain(mixed.at[0, h, :, pl.ds(0, (n_tensor - 1) * HS)], att_recv.at[h])

    def weight_sent():
        for n in range(1, n_tensor):
            @pl.when(t == n - 1)
            def _():
                drain(weight.at[:, pl.ds(0, HS), pl.ds(0, n * w_cols)], up_send)

            @pl.when(t == n_tensor - n)
            def _():
                drain(weight.at[:, pl.ds(0, HS), pl.ds(0, n * w_cols)], down_send)

        drain(weight.at[:, pl.ds(0, HS), :], far_send)
        drain(weight.at[:, pl.ds(0, 2 * HS), :], near_send)

    def part_copy(g, p):
        first, count = bands[g][1:]
        span, cut = pl.ds(first, count), cut_of(p)
        return remote(
            part_out.at[span, cut], part_in.at[span, cut], part_send, part_recv.at[p], device(1 - s, t, b)
        )

    def product(g, h, cut):
        f, first, count = bands[g]
        return jnp.dot(
            mixed[f, h, first : first + count], weight[h, :, cut], preferred_element_type=jnp.float32
        )

    def own_product(h):
        for p in order:
            cut = cut_of(p)
            own_part[:, cut] = product(0, h, cut) if h == 0 else own_part[:, cut] + product(0, h, cut)

    def merge(p):
        cut = cut_of(p)
        drain(part_in.at[:, cut], part_recv.at[p])
        own_part[:, cut] = own_part[:, cut] + part_in[:, cut].astype(jnp.float32)

    def finish(first, last):
        cut = slice(first * w_cols, last * w_cols)
        out_ref[0, :, cut] = (own_part[:, cut] + product(0, heads - 1, cut)).astype(jnp.bfloat16)

    def project_far(g, k):
        first, count = bands[g][1:]
        p = order[k]
        cut = cut_of(p)
        if g == 1:
            drain(weight.at[:, pl.ds(0, 2 * HS), cut], near_recv.at[p])
        part_out[first : first + count, cut] = sum(product(g, h, cut) for h in range(heads)).astype(jnp.bfloat16)
        part_copy(g, p).start()

    def start_far(h, first, last):
        start_kv(h, 0, first, last)
        start_kv(h, 1, first, last)
        start_q(h, 1, first, last)

    for h in range(heads):
        start_kv(h, 1, 0, 1)
        start_q(h, 1, 0, 1)
        start_q(h, 2, 0, 1)

    relay(1)
    inner = 1 + 2 * ((t == 1) | (t == 2)).astype(jnp.int32)
    for h in range(heads):
        start_far(h, 1, inner)
    forward(order[0])
    relay(2)
    for h in range(heads):
        start_far(h, inner, n_tensor)
    forward(order[1])
    relay(3)

    for h in range(heads):
        arrive_kv(h)
        attend(h, 1)
        if h == 0:
            forward(order[2])
        if h == 1:
            forward(order[3])
            for k in range(heads):
                start_q(k, 2, 1, n_tensor)
    start_q(0, 0, 1, n_tensor)
    for h in range(heads):
        arrive_q(h, 2)
        attend(h, 2)
    start_q(1, 0, 1, n_tensor)
    start_q(2, 0, 1, n_tensor)
    back_far(1)
    for k in range(n_tensor):
        project_far(1, k)
    arrive_q(0, 0)
    attend(0, 0)
    back_far(2)
    for k in range(n_tensor):
        project_far(2, k)
    for h in range(1, heads):
        arrive_q(h, 0)
        attend(h, 0)
    weight_sent()
    back_own(0)
    own_product(0)
    back_own(1)
    own_product(1)
    for p in order:
        merge(p)
    back_own(2)
    finish(0, 1)
    finish(1, 2)
    finish(2, 3)
    finish(3, 4)
    drain(got.at[:, :, pl.ds(0, (group - 1) * rows), :], qkv_send)
    drain(done.at[:, pl.ds(0, n_seq * (n_tensor - 1) * rows), :], att_send)
    drain(part_out, part_send)


def fused(axes, sizes, queries, keys, values, lengths, out_weight):
    n_seq, n_tensor, n_bucket = sizes
    rows, width = queries.shape[1:]
    group = n_seq * n_tensor
    heads = width // HS // group
    total = group * rows
    anywhere = pl.BlockSpec(memory_space=pl.ANY)
    dma = pltpu.SemaphoreType.DMA
    return pl.pallas_call(
        functools.partial(whole_kernel, axes, sizes),
        out_shape=jax.ShapeDtypeStruct(queries.shape, queries.dtype),
        in_specs=[pl.BlockSpec(memory_space=pltpu.SMEM), anywhere, anywhere, anywhere, anywhere],
        out_specs=pl.BlockSpec(memory_space=pltpu.VMEM),
        scratch_shapes=[
            pltpu.VMEM((3, rows, width), jnp.bfloat16),
            pltpu.VMEM((heads, 3, total, HS), jnp.bfloat16),
            pltpu.VMEM((heads, total, HS), jnp.bfloat16),
            pltpu.VMEM((n_seq, heads, rows, n_tensor * HS), jnp.bfloat16),
            pltpu.VMEM((heads, n_bucket * HS, width), jnp.bfloat16),
            pltpu.VMEM((rows, width), jnp.bfloat16),
            pltpu.VMEM((rows, width), jnp.bfloat16),
            pltpu.VMEM((rows, width), jnp.float32),
            dma((2,)),
            pltpu.SemaphoreType.REGULAR((3,)),
            dma,
            dma((heads, 3)),
            dma,
            dma((heads + 2,)),
            dma,
            dma,
            dma((n_tensor, heads)),
            dma,
            dma((n_tensor,)),
            dma,
            dma((n_tensor,)),
            dma,
            dma((n_tensor,)),
        ],
        compiler_params=pltpu.CompilerParams(
            collective_id=0, has_side_effects=True, vmem_limit_bytes=32 * 1024 * 1024,
        ),
    )(lengths, *(pltpu.with_memory_space_constraint(x, pltpu.HBM) for x in (queries, keys, values, out_weight)))


def solution(mesh):
    in_specs = (
        P("bucket", ("seq", "tensor"), None),
        P("bucket", ("seq", "tensor"), None),
        P("bucket", ("seq", "tensor"), None),
        P("bucket"),
        P(("seq", "bucket"), "tensor"),
    )
    out_specs = P("bucket", ("seq", "tensor"), None)
    sizes = tuple(mesh.shape[name] for name in ("seq", "tensor", "bucket"))

    def step(queries, keys, values, lengths, out_weight):
        head_count = queries.shape[2] // HS
        fits = sizes[0] == 2 and sizes[1] == sizes[2] == 4 and head_count % (sizes[0] * sizes[1]) == 0
        if fits:
            return fused(mesh.axis_names, sizes, queries, keys, values, lengths, out_weight)
        return shards(queries, keys, values, lengths, out_weight)

    return jax.shard_map(step, mesh=mesh, in_specs=in_specs, out_specs=out_specs, check_vma=False)
```

```python
import functools
import math

import jax
import jax.numpy as jnp
from jax import lax
from jax.experimental import pallas as pl
from jax.experimental.pallas import tpu as pltpu
from jax.sharding import PartitionSpec as P

HS = 128


MASKED_SCORE = -1e30


def shards(queries, keys, values, lengths, out_weight):
    tok_rows = queries.shape[1]
    n_tensor = lax.axis_size("tensor")
    tensor_index = lax.axis_index("tensor")
    live_len = lengths[0]
    local_q, local_k, local_v = (
        lax.all_to_all(queries[0], "seq", split_axis=1, concat_axis=0, tiled=True),
        lax.all_to_all(keys[0], "seq", split_axis=1, concat_axis=0, tiled=True),
        lax.all_to_all(values[0], "seq", split_axis=1, concat_axis=0, tiled=True),
    )
    row_count, col_count = local_q.shape
    head_count = col_count // HS
    query_heads = local_q.reshape(row_count, head_count, HS)

    def spots(first_row, total_rows):
        index_row = first_row + jnp.arange(total_rows, dtype=jnp.int32)
        owner = index_row // row_count
        within = index_row % row_count
        return (within // tok_rows * n_tensor + owner) * tok_rows + within % tok_rows

    query_usable = spots(tensor_index * row_count, row_count) < live_len
    initial = (
        jnp.full((row_count, head_count), MASKED_SCORE, jnp.float32),
        jnp.zeros((row_count, head_count), jnp.float32),
        jnp.zeros((row_count, head_count, HS), jnp.float32),
    )
    carried = initial
    first_row = jnp.int32(0)
    key_rows = lax.all_gather(local_k, "tensor", axis=0, tiled=True)
    value_rows = lax.all_gather(local_v, "tensor", axis=0, tiled=True)
    for offset in range(key_rows.shape[0] // row_count):
        row_peak, row_sum, accumulated = carried
        key_tile = key_rows[offset * row_count : (offset + 1) * row_count].reshape(
            row_count, head_count, HS
        )
        value_tile = value_rows[offset * row_count : (offset + 1) * row_count].reshape(
            row_count, head_count, HS
        )
        key_usable = spots(first_row + offset * row_count, row_count) < live_len
        scores = jnp.einsum(
            "qhd,khd->qhk", query_heads, key_tile, preferred_element_type=jnp.float32
        ) * HS ** (-0.5)
        scores = jnp.where(key_usable[None, None, :], scores, MASKED_SCORE)
        peak_new = jnp.maximum(row_peak, jnp.max(scores, axis=-1))
        exponent = jnp.where(key_usable[None, None, :], jnp.exp(scores - peak_new[..., None]), 0.0)
        rescale = jnp.exp(row_peak - peak_new)
        accumulated = accumulated * rescale[..., None] + jnp.einsum(
            "qhk,khd->qhd",
            exponent.astype(jnp.bfloat16),
            value_tile,
            preferred_element_type=jnp.float32,
        )
        carried = (peak_new, row_sum * rescale + jnp.sum(exponent, axis=-1), accumulated)
    row_peak, row_sum, accumulated = carried
    attended = accumulated / row_sum[..., None]
    mixed = jnp.where(query_usable[:, None], attended.reshape(row_count, col_count), 0.0).astype(
        jnp.bfloat16
    )
    restored = lax.all_to_all(mixed, "seq", split_axis=0, concat_axis=1, tiled=True)
    wide_weight = lax.all_gather(out_weight, "tensor", axis=1, tiled=True)
    summed = jnp.dot(
        restored,
        lax.all_gather(wide_weight, ("seq", "bucket"), axis=0, tiled=True),
        preferred_element_type=jnp.float32,
    )
    return summed.astype(jnp.bfloat16)[None]


def whole_kernel(
    axes, sizes, len_ref, q_ref, k_ref, v_ref, w_ref, out_ref,
    held, got, done, mixed, weight, part_out, part_in, own_part, load_sem, ready,
    qkv_send, qkv_recv, att_send, att_recv, up_send, down_send, line_recv,
    far_send, far_recv, near_send, near_recv, part_send, part_recv,
):
    n_seq, n_tensor, n_bucket = sizes
    s, t, b = lax.axis_index("seq"), lax.axis_index("tensor"), lax.axis_index("bucket")
    group = n_seq * n_tensor
    rows = q_ref.shape[1]
    width = q_ref.shape[2]
    heads = width // HS // group
    w_rows, w_cols = w_ref.shape

    def device(ds, dt, db):
        place = {"seq": ds, "tensor": dt, "bucket": db}
        return tuple(place[name] for name in axes)

    def remote(src, dst, send, recv, where):
        return pltpu.make_async_remote_copy(
            src_ref=src, dst_ref=dst, send_sem=send, recv_sem=recv,
            device_id=where, device_id_type=pl.DeviceIdType.MESH,
        )

    me = s * n_tensor + t
    streams = (q_ref, k_ref, v_ref)
    barrier = pltpu.get_barrier_semaphore()

    def spot(place):
        return pl.ds(pl.multiple_of(place * rows, rows), rows)

    toward = 1 - 2 * (t // (n_tensor // 2))

    def along(i):
        return (t + toward * i + 2 * n_tensor) % n_tensor

    def drain(ref, sem):
        pltpu.make_async_copy(ref, ref, sem).wait()

    part_rows = rows // 2
    bands = ((0, 0, rows), (1, 0, part_rows), (1, part_rows, part_rows))

    def band_rows(g, place):
        f, first, count = bands[g]
        return pl.ds(pl.multiple_of(place * rows + first, part_rows), count)

    def send_copy(h, j, i, f, g):
        dt = along(i)
        ds = (s + f) % 2
        cols = pl.ds(pl.multiple_of(((ds * n_tensor + dt) * heads + h) * HS, HS), HS)
        first, count = (0, rows) if j else bands[g][1:]
        return remote(
            held.at[j, pl.ds(first, count), cols],
            got.at[h, j, pl.ds(pl.multiple_of(me * rows + first, part_rows), count), :],
            qkv_send,
            qkv_recv.at[h, 1 if j else g],
            device(ds, dt, b),
        )

    def start_kv(h, f, first, last):
        def body(i, carry):
            for j in (1, 2):
                send_copy(h, j, i, f, 0).start()
            return carry

        lax.fori_loop(first, last, body, 0)

    def start_q(h, g, first, last):
        def body(i, carry):
            send_copy(h, 0, i, bands[g][0], g).start()
            return carry

        lax.fori_loop(first, last, body, 0)

    def arrive_kv(h):
        drain(got.at[h, :, pl.ds(0, (2 * group * rows + n_tensor * part_rows) // 3), :], qkv_recv.at[h, 1])

    def arrive_q(h, g):
        drain(got.at[h, 0, pl.ds(0, n_tensor * bands[g][2]), :], qkv_recv.at[h, g])

    def piece(row_block, col_block, c):
        return weight.at[
            c,
            pl.ds(pl.multiple_of(row_block * HS, HS), HS),
            pl.ds(pl.multiple_of(col_block * w_cols, w_cols), w_cols),
        ]

    def cut_of(p):
        return pl.ds(pl.multiple_of(p * w_cols, w_cols), w_cols)

    far, near = (b + 2) % 4, b + 1 - 2 * (b % 2)

    def up_copy(p, c):
        return remote(
            piece(b, p, c), piece(b, p, c), up_send, line_recv.at[p, c], device(s, t + 1, b)
        )

    def down_copy(p, c):
        return remote(
            piece(b, p, c), piece(b, p, c), down_send, line_recv.at[p, c], device(s, t - 1, b)
        )

    def far_copy(p, c, row_block):
        return remote(
            piece(row_block, p, c), piece(row_block, p, c), far_send, far_recv.at[p], device(s, t, far)
        )

    def near_copy(p, c, row_block):
        return remote(
            piece(row_block, p, c), piece(row_block, p, c), near_send, near_recv.at[p], device(s, t, near)
        )

    def spread(p, c):
        far_copy(p, c, b).start()
        near_copy(p, c, b).start()

    def relay_chunk(k, c):
        @pl.when(t >= k)
        def _():
            up_copy(t - k, c).wait_recv()

            @pl.when(t < n_tensor - 1)
            def _():
                up_copy(t - k, c).start()

            spread(t - k, c)

        @pl.when(t + k < n_tensor)
        def _():
            down_copy(t + k, c).wait_recv()

            @pl.when(t > 0)
            def _():
                down_copy(t + k, c).start()

            spread(t + k, c)

    def relay(k):
        for c in range(heads):
            relay_chunk(k, c)

    def weight_load(c):
        return pltpu.make_async_copy(w_ref.at[pl.ds(c * HS, HS), :], piece(b, t, c), load_sem.at[1])

    def load(j):
        return pltpu.make_async_copy(streams[j].at[0], held.at[j], load_sem.at[0])

    def own_copy(h, j):
        cols = pl.ds(pl.multiple_of((me * heads + h) * HS, HS), HS)
        return pltpu.make_async_copy(
            streams[j].at[0, :, cols], got.at[h, j, spot(me), :], qkv_recv.at[h, 1 if j else 0]
        )

    def greet(semaphore, where):
        pl.semaphore_signal(semaphore, inc=1, device_id=where, device_id_type=pl.DeviceIdType.MESH)

    def greet_group(semaphore):
        greet(semaphore, device(1 - s, t, b))

        @pl.when(t > 0)
        def _():
            greet(semaphore, device(s, t - 1, b))

        @pl.when(t < n_tensor - 1)
        def _():
            greet(semaphore, device(s, t + 1, b))

    beside = 1 + (t > 0).astype(jnp.int32) + (t < n_tensor - 1).astype(jnp.int32)
    greet_group(barrier)
    greet(barrier, device(s, t, far))
    greet(barrier, device(s, t, near))
    for c in range(heads):
        weight_load(c).start()
    pl.semaphore_wait(barrier, beside + 2)
    drain(weight.at[:, pl.ds(pl.multiple_of(b * HS, HS), HS), cut_of(t)], load_sem.at[1])

    for c in range(heads):
        @pl.when(t < n_tensor - 1)
        def _():
            up_copy(t, c).start()

        @pl.when(t > 0)
        def _():
            down_copy(t, c).start()

        spread(t, c)
    for j in (1, 2, 0):
        load(j).start()
    for h in range(heads):
        for j in range(3):
            own_copy(h, j).start()
    for k in range(3):
        greet_group(ready.at[k])
        pl.semaphore_wait(ready.at[k], beside)
    drain(held, load_sem.at[0])
    live = len_ref[0]

    upper = t // 2
    order = (t, 1 - t + 4 * upper, 2 - upper, 3 - 3 * upper)

    def forward(p):
        drain(weight.at[:, pl.ds(pl.multiple_of(far * HS, HS), HS), cut_of(p)], far_recv.at[p])
        for c in range(heads):
            near_copy(p, c, far).start()

    total = group * rows
    usable = lax.broadcasted_iota(jnp.int32, (1, total), 1) < live
    factor = HS ** (-0.5) * math.log2(math.e)

    def att_copy(h, g, target):
        f, first, count = bands[g]
        return remote(
            done.at[h, band_rows(g, (s + f) % 2 * n_tensor + target), :],
            mixed.at[f, h, pl.ds(first, count), pl.ds(pl.multiple_of(t * HS, HS), HS)],
            att_send, att_recv.at[heads + g - 1 if f else h], device(s, target, b),
        )

    def attend_rows(h, query, own_token):
        scores = lax.dot_general(
            query, got[h, 1], (((1,), (1,)), ((), ())), preferred_element_type=jnp.float32
        )
        scores = jnp.where(usable, scores, MASKED_SCORE)
        peak = jnp.max(scores, axis=-1, keepdims=True)
        expo = jnp.exp2((scores - peak) * factor)
        denominator = jnp.sum(expo, axis=-1, keepdims=True)
        result = jnp.dot(expo.astype(jnp.bfloat16), got[h, 2], preferred_element_type=jnp.float32) / denominator
        return jnp.where(own_token < live, result, 0.0).astype(jnp.bfloat16)

    def attend(h, g):
        f, first, count = bands[g]
        side = (s + f) % 2 * n_tensor
        row = first + lax.broadcasted_iota(jnp.int32, (count, 1), 0)
        together = 2 * rows // count
        for step in range(0, n_tensor, together):
            targets = [along(step + i + 1 if g or step + i + 1 == n_tensor else n_tensor - 1 - step - i) for i in range(together)]
            spans = [band_rows(g, side + target) for target in targets]
            result = attend_rows(
                h,
                jnp.concatenate([got[h, 0, span, :] for span in spans], axis=0),
                jnp.concatenate([(side + target) * rows + row for target in targets], axis=0),
            )
            for i in range(together):
                piece_rows = result[i * count : (i + 1) * count]
                if step + i + 1 < n_tensor:
                    done[h, spans[i], :] = piece_rows
                    att_copy(h, g, targets[i]).start()
                else:
                    mixed[f, h, pl.ds(first, count), pl.ds(pl.multiple_of(t * HS, HS), HS)] = piece_rows

    def back_far(g):
        drain(mixed.at[1, :, pl.ds(0, part_rows), pl.ds(0, (n_tensor - 1) * HS)], att_recv.at[heads + g - 1])

    def back_own(h):
        drain(mixed.at[0, h, :, pl.ds(0, (n_tensor - 1) * HS)], att_recv.at[h])

    def weight_sent():
        for n in range(1, n_tensor):
            @pl.when(t == n - 1)
            def _():
                drain(weight.at[:, pl.ds(0, HS), pl.ds(0, n * w_cols)], up_send)

            @pl.when(t == n_tensor - n)
            def _():
                drain(weight.at[:, pl.ds(0, HS), pl.ds(0, n * w_cols)], down_send)

        drain(weight.at[:, pl.ds(0, HS), :], far_send)
        drain(weight.at[:, pl.ds(0, 2 * HS), :], near_send)

    def part_copy(g, p):
        first, count = bands[g][1:]
        span, cut = pl.ds(first, count), cut_of(p)
        return remote(
            part_out.at[span, cut], part_in.at[span, cut], part_send, part_recv.at[p], device(1 - s, t, b)
        )

    def product(g, h, cut):
        f, first, count = bands[g]
        return jnp.dot(
            mixed[f, h, first : first + count], weight[h, :, cut], preferred_element_type=jnp.float32
        )

    def own_product(h):
        for p in order:
            cut = cut_of(p)
            own_part[:, cut] = product(0, h, cut) if h == 0 else own_part[:, cut] + product(0, h, cut)

    def merge(p):
        cut = cut_of(p)
        drain(part_in.at[:, cut], part_recv.at[p])
        own_part[:, cut] = own_part[:, cut] + part_in[:, cut].astype(jnp.float32)

    def finish(first, last):
        cut = slice(first * w_cols, last * w_cols)
        out_ref[0, :, cut] = (own_part[:, cut] + product(0, heads - 1, cut)).astype(jnp.bfloat16)

    def project_far(g, k):
        first, count = bands[g][1:]
        p = order[k]
        cut = cut_of(p)
        if g == 1:
            drain(weight.at[:, pl.ds(0, 2 * HS), cut], near_recv.at[p])
        part_out[first : first + count, cut] = sum(product(g, h, cut) for h in range(heads)).astype(jnp.bfloat16)
        part_copy(g, p).start()

    def start_far(h, first, last):
        start_kv(h, 0, first, last)
        start_kv(h, 1, first, last)
        start_q(h, 1, first, last)

    for h in range(heads):
        start_kv(h, 1, 0, 1)
        start_q(h, 1, 0, 1)
        start_q(h, 2, 0, 1)

    relay(1)
    held_back = 1 + 2 * ((t == 1) | (t == 2)).astype(jnp.int32) * (1 - b % 2)
    inner = 1 + 2 * ((t == 1) | (t == 2)).astype(jnp.int32)
    for h in range(heads):
        start_far(h, 1, inner if h < 2 else held_back)
    forward(order[0])
    relay(2)
    for h in range(heads):
        start_far(h, inner if h < 2 else held_back, n_tensor)
    forward(order[1])
    relay(3)

    for h in range(heads):
        arrive_kv(h)
        attend(h, 1)
        if h == 0:
            forward(order[2])
        if h == 1:
            forward(order[3])
            for k in range(heads):
                start_q(k, 2, 1, n_tensor)
    start_q(0, 0, 1, n_tensor)
    for h in range(heads):
        arrive_q(h, 2)
        attend(h, 2)
    start_q(1, 0, 1, n_tensor)
    start_q(2, 0, 1, n_tensor)
    back_far(1)
    for k in range(n_tensor):
        project_far(1, k)
    arrive_q(0, 0)
    attend(0, 0)
    back_far(2)
    for k in range(n_tensor):
        project_far(2, k)
    for h in range(1, heads):
        arrive_q(h, 0)
        attend(h, 0)
    weight_sent()
    back_own(0)
    own_product(0)
    back_own(1)
    own_product(1)
    for p in order:
        merge(p)
    back_own(2)
    finish(0, 1)
    finish(1, 2)
    finish(2, 3)
    finish(3, 4)
    drain(got.at[:, :, pl.ds(0, (group - 1) * rows), :], qkv_send)
    drain(done.at[:, pl.ds(0, n_seq * (n_tensor - 1) * rows), :], att_send)
    drain(part_out, part_send)


def fused(axes, sizes, queries, keys, values, lengths, out_weight):
    n_seq, n_tensor, n_bucket = sizes
    rows, width = queries.shape[1:]
    group = n_seq * n_tensor
    heads = width // HS // group
    total = group * rows
    anywhere = pl.BlockSpec(memory_space=pl.ANY)
    dma = pltpu.SemaphoreType.DMA
    return pl.pallas_call(
        functools.partial(whole_kernel, axes, sizes),
        out_shape=jax.ShapeDtypeStruct(queries.shape, queries.dtype),
        in_specs=[pl.BlockSpec(memory_space=pltpu.SMEM), anywhere, anywhere, anywhere, anywhere],
        out_specs=pl.BlockSpec(memory_space=pltpu.VMEM),
        scratch_shapes=[
            pltpu.VMEM((3, rows, width), jnp.bfloat16),
            pltpu.VMEM((heads, 3, total, HS), jnp.bfloat16),
            pltpu.VMEM((heads, total, HS), jnp.bfloat16),
            pltpu.VMEM((n_seq, heads, rows, n_tensor * HS), jnp.bfloat16),
            pltpu.VMEM((heads, n_bucket * HS, width), jnp.bfloat16),
            pltpu.VMEM((rows, width), jnp.bfloat16),
            pltpu.VMEM((rows, width), jnp.bfloat16),
            pltpu.VMEM((rows, width), jnp.float32),
            dma((2,)),
            pltpu.SemaphoreType.REGULAR((3,)),
            dma,
            dma((heads, 3)),
            dma,
            dma((heads + 2,)),
            dma,
            dma,
            dma((n_tensor, heads)),
            dma,
            dma((n_tensor,)),
            dma,
            dma((n_tensor,)),
            dma,
            dma((n_tensor,)),
        ],
        compiler_params=pltpu.CompilerParams(
            collective_id=0, has_side_effects=True, vmem_limit_bytes=32 * 1024 * 1024,
        ),
    )(lengths, *(pltpu.with_memory_space_constraint(x, pltpu.HBM) for x in (queries, keys, values, out_weight)))


def solution(mesh):
    in_specs = (
        P("bucket", ("seq", "tensor"), None),
        P("bucket", ("seq", "tensor"), None),
        P("bucket", ("seq", "tensor"), None),
        P("bucket"),
        P(("seq", "bucket"), "tensor"),
    )
    out_specs = P("bucket", ("seq", "tensor"), None)
    sizes = tuple(mesh.shape[name] for name in ("seq", "tensor", "bucket"))

    def step(queries, keys, values, lengths, out_weight):
        head_count = queries.shape[2] // HS
        fits = sizes[0] == 2 and sizes[1] == sizes[2] == 4 and head_count % (sizes[0] * sizes[1]) == 0
        if fits:
            return fused(mesh.axis_names, sizes, queries, keys, values, lengths, out_weight)
        return shards(queries, keys, values, lengths, out_weight)

    return jax.shard_map(step, mesh=mesh, in_specs=in_specs, out_specs=out_specs, check_vma=False)
```
